128 devices in a mesh: aa: 16 (over z_hi, x, core), ba: 8 (over z_lo, y).
Axes of the slice: x: 4, y: 4, z: 4 (z_hi: 2, z_lo: 2; z = z_hi * 2 + z_lo), core: 2. Of those that a mesh axis runs over, the one named last changes fastest.
Arguments:
- images: float32 [128, 4, 128, 4096], P(('aa', 'ba')), may hold values from 0 to 0.06, as said below
- depth: int32 [128], replicated, may hold values from 0 to 127, as said below
- brick_map: int32 [128], replicated, may hold values from 0 to 127, as said below
Outputs:
- composite: float32 [4, 128, 4096], replicated
The draws below stay inside these ranges and needn't reach their ends.
Inputs may be any that keep to these rules, and one draw needn't show every extreme that they name: depth: a permutation of 0 to 127; the devices that share one index of ba hold bricks of 16 consecutive depth ranks. brick_map: a permutation of 0 to 127. images: channel 3 (alpha) lies between 0.002 and 0.06; channels 0 to 2 lie between 0 and the pixel's alpha.
All inputs are finite; a program needn't handle non-finite values.
Results may differ from the reference program's by a relative error of at most 0.00002.
Values sent between devices are 32-bit elements; how exact they have to be, the bound alone decides.
A program may use at most 128 MiB of HBM per device.

```python
import jax
import jax.numpy as jnp
from jax import lax

COLUMNS = 4096
ROWS = 128
N_AA = 16
N_BA = 8
DEVICES = 128


def order_tables(key):
    base = jax.random.fold_in(key, 7)
    key_group, key_inner, key_brick = jax.random.split(base, 3)
    group_slot = jax.random.permutation(key_group, N_BA).astype(jnp.int32)
    inner_keys = jax.random.split(key_inner, N_BA)
    inner = jax.vmap(lambda single: jax.random.permutation(single, N_AA))(inner_keys).astype(jnp.int32)
    device_rank = (group_slot[None, :] * N_AA + inner.T).reshape(DEVICES)
    brick_map = jax.random.permutation(key_brick, DEVICES).astype(jnp.int32)
    depth = jnp.zeros((DEVICES,), jnp.int32).at[brick_map].set(device_rank)
    return (depth, brick_map)


def draw_depth(key, part):
    return order_tables(key)[0]


def draw_brick_map(key, part):
    return order_tables(key)[1]


def draw_images(key, part):
    key_alpha, key_color = jax.random.split(jax.random.fold_in(key, 11), 2)
    shape = (DEVICES, 1, ROWS, COLUMNS)
    alpha = jnp.exp(jax.random.uniform(key_alpha, shape, jnp.float32, jnp.log(0.002), jnp.log(0.06)))
    color = alpha * jax.random.uniform(key_color, (DEVICES, 3, ROWS, COLUMNS), jnp.float32, 0.0, 1.0)
    return jnp.concatenate([color, alpha], axis=1).astype(jnp.float32)


def setup_inputs(seed: int = 0) -> dict:
    keys = jax.random.split(jax.random.key(seed), 4)
    images = draw_images(jax.random.fold_in(keys[3], 71), 0)
    depth = draw_depth(jax.random.fold_in(keys[3], 71), 0)
    brick_map = draw_brick_map(jax.random.fold_in(keys[3], 71), 0)
    return {"images": images, "depth": depth, "brick_map": brick_map}


def reference(images, depth, brick_map):
    device_rank = depth[brick_map].astype(jnp.int32)
    ordering = jnp.argsort(device_rank).astype(jnp.int32)

    def blend_step(total, index):
        piece = images[index]
        return total + (1.0 - total[3:4]) * piece, None

    start = jnp.zeros(images.shape[1:], jnp.float32)
    composite, unused = lax.scan(blend_step, start, ordering)
    return composite
```

```python
import functools

import jax
import jax.numpy as jnp
from jax import lax
from jax.experimental import pallas as pl
from jax.experimental.pallas import tpu as pltpu
from jax.sharding import Mesh
from jax.sharding import PartitionSpec as P

AXES = ("zh", "x", "c", "zl", "y")
CHUNKS = 4
ROW = 8
MESH = pl.DeviceIdType.MESH

AA_ORDER = [(dx, dz, dc) for dc in (0, 1) for dx, dz in
            ((1, 1), (3, 1), (0, 1), (2, 1), (1, 0), (3, 0), (2, 0), (0, 0))][:]
AA_ORDER = [p for p in AA_ORDER if p != (0, 0, 0)]
BA_ORDER = [(dy, dz) for dy in (2, 1, 3, 0) for dz in (1, 0) if (dy, dz) != (0, 0)]
XZ_ORDER = [(dx, dz) for dx, dz in
            ((2, 2), (1, 2), (3, 2), (2, 1), (2, 3), (1, 1), (3, 3), (1, 3), (3, 1),
             (0, 2), (2, 0), (1, 0), (0, 1), (3, 0), (0, 3))]

TIMES = {
    "prefix": (7, 7), "group": (12, 7), "trans": (16, 7), "scale": (37, 7), "sum_core": (40, 7),
    "sum_y": (49, 8), "sum_xz": (56, 8), "gather_y": (62, 9), "gather_core": (73, 10), "finish": (78, 10),
}


def kernel(tab, img, out, *scratch):
    ain, gin = scratch[:CHUNKS], scratch[CHUNKS:2 * CHUNKS]
    pre, gb, qb, qout, qin, tout, tin, col, cs, cin, a1, yin, a2, xin, send, recv, own = scratch[2 * CHUNKS:]
    zh, x, c, zl, y = (lax.axis_index(a) for a in AXES)
    z = zh * 2 + zl
    width = tin.shape[-1]
    tile = width // 8
    quarter = width // 4
    band = c * 8 + zh * 4 + x
    slot_b = y * 2 + zl

    def remote(src, dst, stage, k, device):
        cp = pltpu.make_async_remote_copy(
            src_ref=src, dst_ref=dst, send_sem=send.at[stage, k], recv_sem=recv.at[stage, k],
            device_id=device, device_id_type=MESH)
        cp.start()

    def arrived(ref, stage, k):
        pltpu.make_async_copy(ref, ref, recv.at[stage, k]).wait()

    def sent(ref, stage, k):
        pltpu.make_async_copy(ref, ref, send.at[stage, k]).wait()

    def aa_peers():
        for dx, dz, dc in AA_ORDER:
            xx, zz, cc = lax.rem(x + dx, 4), lax.rem(zh + dz, 2), lax.rem(c + dc, 2)
            yield cc * 8 + zz * 4 + xx, (zz, xx, cc, zl, y)

    def ba_peers():
        for dy, dz in BA_ORDER:
            yy, zz = lax.rem(y + dy, 4), lax.rem(zl + dz, 2)
            yield yy * 2 + zz, (zh, x, c, zz, yy)

    def xz_peers():
        for n, (dx, dz) in enumerate(XZ_ORDER):
            xx, zz = lax.rem(x + dx, 4), lax.rem(z + dz, 4)
            yield n, zz // 2 * 4 + xx, lax.rem(zz, 2), (zz // 2, xx, c, lax.rem(zz, 2), y)

    def y_peers():
        for n, dy in enumerate((2, 1, 3)):
            yy = lax.rem(y + dy, 4)
            yield n, yy, (zh, x, c, zl, yy)

    partner = (zh, x, 1 - c, zl, y)

    def cols(k):
        return pl.ds(k * width, width)

    def own_alpha(k):
        return pltpu.make_async_copy(img.at[3, band, :, cols(k)], ain[k].at[band], own.at[0, k])

    def own_color(k):
        return pltpu.make_async_copy(img.at[pl.ds(0, 3), :, :, cols(k)], col.at[k], own.at[1, k])

    def alpha(k):
        for r, device in aa_peers():
            remote(img.at[3, r, :, cols(k)], ain[k].at[band], 0, k, device)
        own_alpha(k).start()

    def prefix(k):
        own_alpha(k).wait()
        arrived(ain[k].at[pl.ds(0, 15)], 0, k)
        run = jnp.ones((ROW, width), jnp.float32)
        for m in range(16):
            pre[k, m] = run
            run = run * (1.0 - ain[k][tab[m]])
        for j in range(8):
            gb[k, j] = run[:, j * tile:(j + 1) * tile]
        gin[k][slot_b] = gb[k, slot_b]
        for j, device in ba_peers():
            remote(gb.at[k, j], gin[k].at[slot_b], 1, k, device)

    def group(k):
        arrived(gin[k].at[pl.ds(0, 7)], 1, k)
        run = jnp.ones((ROW, tile), jnp.float32)
        for m in range(8):
            qb[k, m] = run
            run = run * gin[k][tab[32 + m]]
        out[3, band, :, pl.ds(pl.multiple_of(k * width + slot_b * tile, 128), tile)] = 1.0 - run
        for j in range(8):
            qout[k, j] = qb[k, tab[40 + j]]
        qin[k, slot_b] = qout[k, slot_b]
        for j, device in ba_peers():
            remote(qout.at[k, j], qin.at[k, slot_b], 2, k, device)

    def trans(k):
        arrived(qin.at[k, pl.ds(0, 7)], 2, k)
        q = jnp.concatenate([qin[k, j] for j in range(8)], axis=1)
        for r in range(16):
            tout[k, r] = pre[k, tab[16 + r]] * q
        tin[k, band] = tout[k, band]
        for r, device in aa_peers():
            remote(tout.at[k, r], tin.at[k, band], 3, k, device)

    def scale(k):
        own_color(k).wait()
        arrived(tin.at[k, pl.ds(0, 15)], 3, k)

        def body(i, carry):
            r = (1 - c) * 8 + i
            t = tin[k, r]
            for ch in range(3):
                cs[k, ch, i] = col[k, ch, r] * t
            return carry

        lax.fori_loop(0, 8, body, 0)
        remote(cs.at[k], cin.at[k], 4, k, partner)

    def sum_core(k):
        arrived(cin.at[k], 4, k)

        def body(i, carry):
            r = c * 8 + i
            t = tin[k, r]
            for ch in range(3):
                a1[k, ch, i] = col[k, ch, r] * t + cin[k, ch, i]
            return carry

        lax.fori_loop(0, 8, body, 0)
        for n, yy, device in y_peers():
            at = pl.ds(pl.multiple_of(yy * quarter, 128), quarter)
            remote(a1.at[k, :, :, :, at], yin.at[k, n], 5, k, device)

    def sum_y(k):
        arrived(yin.at[k], 5, k)

        def body(i, carry):
            at = pl.ds(pl.multiple_of(y * quarter, 128), quarter)
            for ch in range(3):
                a2[k, ch, i] = a1[k, ch, i, :, at] + yin[k, 0, ch, i] + (yin[k, 1, ch, i] + yin[k, 2, ch, i])
            return carry

        lax.fori_loop(0, 8, body, 0)
        for n, r, t, device in xz_peers():
            at = pl.ds(pl.multiple_of(t * tile, 128), tile)
            remote(a2.at[k, :, r, :, at], xin.at[k, n], 6, k, device)

    def strip(k):
        return pl.ds(pl.multiple_of(k * width + slot_b * tile, 128), tile)

    def sum_xz(k):
        arrived(xin.at[k], 6, k)
        at = pl.ds(pl.multiple_of(zl * tile, 128), tile)
        for ch in range(3):
            s = a2[k, ch, zh * 4 + x, :, at]
            for n in range(15):
                s = s + xin[k, n, ch]
            out[ch, band, :, strip(k)] = s
        mine = out.at[:, band, :, strip(k)]
        for n, r, t, device in xz_peers():
            remote(mine, mine, 7, k, device)

    def piece(k, yy, cc):
        return out.at[:, pl.ds(pl.multiple_of(cc * 8, 8), 8), :, pl.ds(pl.multiple_of(k * width + yy * quarter, 128), quarter)]

    def gather_y(k):
        arrived(xin_like(k), 7, k)
        mine = piece(k, y, c)
        for n, yy, device in y_peers():
            remote(mine, mine, 8, k, device)
        remote(mine, mine, 9, k, partner)

    def xin_like(k):
        return out.at[:, pl.ds(0, 15), :, pl.ds(0, tile)]

    def gather_core(k):
        arrived(out.at[pl.ds(0, 3), pl.ds(0, 8), :, pl.ds(0, width)], 8, k)
        for n, yy, device in y_peers():
            mine = piece(k, yy, c)
            remote(mine, mine, 9, k, partner)

    def finish(k):
        arrived(out.at[:, pl.ds(0, 8), :, pl.ds(0, width)], 9, k)
        sent(ain[k].at[pl.ds(0, 15)], 0, k)
        sent(gb.at[k, pl.ds(0, 7)], 1, k)
        sent(qout.at[k, pl.ds(0, 7)], 2, k)
        sent(tout.at[k, pl.ds(0, 15)], 3, k)
        sent(cs.at[k], 4, k)
        sent(yin.at[k], 5, k)
        sent(xin.at[k], 6, k)
        sent(xin_like(k), 7, k)
        sent(out.at[pl.ds(0, 3), pl.ds(0, 8), :, pl.ds(0, width)], 8, k)
        sent(out.at[:, pl.ds(0, 8), :, pl.ds(0, width)], 9, k)

    stages = dict(prefix=prefix, group=group, trans=trans, scale=scale, sum_core=sum_core, sum_y=sum_y,
                  sum_xz=sum_xz, gather_y=gather_y, gather_core=gather_core, finish=finish)
    for k in range(CHUNKS):
        alpha(k)
    for k in range(CHUNKS):
        own_color(k).start()
    names = list(stages)
    plan = sorted((TIMES[s][0] + TIMES[s][1] * k, names.index(s), k) for s in names for k in range(CHUNKS))
    for when, s, k in plan:
        stages[names[s]](k)


def tables(depth, brick_map):
    count = depth.shape[0]
    bricks = jnp.arange(count, dtype=jnp.int32)
    rank = jnp.sum(jnp.where(brick_map[:, None] == bricks[None, :], depth[None, :], 0), axis=1)
    rank = rank.reshape(2, 4, 2, 2, 4)
    group = rank[0, 0, 0] // 16
    group = group.T.reshape(8)
    zl, y = lax.axis_index("zl"), lax.axis_index("y")
    inner = lax.dynamic_slice(rank, (0, 0, 0, zl, y), (2, 4, 2, 1, 1)).reshape(2, 4, 2) % 16
    inner = inner.transpose(2, 0, 1).reshape(16)

    def inverse(r, n):
        i = jnp.arange(n, dtype=jnp.int32)
        return jnp.sum(jnp.where(r[None, :] == i[:, None], i[None, :], 0), axis=1)

    return jnp.concatenate([inverse(inner, 16), inner, inverse(group, 8), group]).astype(jnp.int32)


def local(images, depth, brick_map):
    channels, rows, columns = images.shape[1:]
    tab = tables(depth, brick_map)
    width = columns // CHUNKS
    tile, quarter = width // 8, width // 4
    f = jnp.float32
    n = CHUNKS
    vm = lambda *s: pltpu.VMEM(s, f)
    out = pl.pallas_call(
        kernel,
        out_shape=jax.ShapeDtypeStruct((channels, rows // ROW, ROW, columns), f),
        in_specs=[pl.BlockSpec(memory_space=pltpu.SMEM), pl.BlockSpec(memory_space=pl.ANY)],
        out_specs=pl.BlockSpec(memory_space=pltpu.VMEM),
        scratch_shapes=[
            *[vm(16, ROW, width)] * n, *[vm(8, ROW, tile)] * n,
            vm(n, 16, ROW, width), vm(n, 8, ROW, tile), vm(n, 8, ROW, tile), vm(n, 8, ROW, tile), vm(n, 8, ROW, tile),
            vm(n, 16, ROW, width), vm(n, 16, ROW, width),
            vm(n, 3, 16, ROW, width), vm(n, 3, 8, ROW, width), vm(n, 3, 8, ROW, width), vm(n, 3, 8, ROW, width),
            vm(n, 3, 3, 8, ROW, quarter), vm(n, 3, 8, ROW, quarter), vm(n, 15, 3, ROW, tile),
            pltpu.SemaphoreType.DMA((10, n)), pltpu.SemaphoreType.DMA((10, n)), pltpu.SemaphoreType.DMA((2, n)),
        ],
        compiler_params=pltpu.CompilerParams(has_side_effects=True, vmem_limit_bytes=60 * 2**20),
    )(tab, images.reshape(channels, rows // ROW, ROW, columns))
    return out.reshape(channels, rows, columns)


def solution(mesh):
    torus = Mesh(mesh.devices.reshape(2, 4, 2, 2, 4), AXES)
    return jax.shard_map(
        local,
        mesh=torus,
        in_specs=(P(("zh", "x", "c", "zl", "y"), None, None, None), P(), P()),
        out_specs=P(),
        check_vma=False,
    )
```

```python
import functools

import jax
import jax.numpy as jnp
from jax import lax
from jax.experimental import pallas as pl
from jax.experimental.pallas import tpu as pltpu
from jax.sharding import Mesh
from jax.sharding import PartitionSpec as P

AXES = ("zh", "x", "c", "zl", "y")
CHUNKS = 4
ROW = 8
MESH = pl.DeviceIdType.MESH

AA_ORDER = [(dx, dz, dc) for dc in (0, 1) for dx, dz in
            ((1, 1), (3, 1), (0, 1), (2, 1), (1, 0), (3, 0), (2, 0), (0, 0))][:]
AA_ORDER = [p for p in AA_ORDER if p != (0, 0, 0)]
BA_ORDER = [(dy, dz) for dy in (2, 1, 3, 0) for dz in (1, 0) if (dy, dz) != (0, 0)]
XZ_ORDER = [(dx, dz) for dx, dz in
            ((2, 2), (1, 2), (3, 2), (2, 1), (2, 3), (1, 1), (3, 3), (1, 3), (3, 1),
             (0, 2), (2, 0), (1, 0), (0, 1), (3, 0), (0, 3))]

PLAN = (
    "alpha0", "alpha1", "load", "prefix0", "alpha2", "group0", "prefix1", "alpha3", "trans0", "group1",
    "prefix2", "trans1", "group2", "prefix3", "trans2", "scale0", "sum_core0", "group3", "trans3", "around0",
    "scale1", "sum_core1", "sum_y0", "around1", "sum_xz0", "gather_y0", "sum_y1", "scale2", "sum_core2",
    "forward0", "sum_xz1", "around2", "gather_core0", "gather_y1", "scale3", "sum_core3", "sum_y2",
    "forward1", "around3", "sum_xz2", "gather_core1", "gather_y2", "sum_y3", "sum_xz3", "forward2",
    "gather_y3", "gather_core2", "forward3", "gather_core3", "finish",
)


def kernel(depth, bricks, img, out, *scratch):
    ain, gin = scratch[:CHUNKS], scratch[CHUNKS:2 * CHUNKS]
    pre, gb, qb, qout, qin, tout, tin, col, cs, cin, a1, ys, b1, yin, a2, xin, send, recv, own = scratch[2 * CHUNKS:]
    zh, x, c, zl, y = (lax.axis_index(a) for a in AXES)
    z = zh * 2 + zl
    width = tin.shape[-1]
    tile = width // 8
    quarter = width // 4
    band = c * 8 + zh * 4 + x
    slot_b = y * 2 + zl

    def remote(src, dst, stage, k, device):
        cp = pltpu.make_async_remote_copy(
            src_ref=src, dst_ref=dst, send_sem=send.at[stage, k], recv_sem=recv.at[stage, k],
            device_id=device, device_id_type=MESH)
        cp.start()

    def arrived(ref, stage, k):
        pltpu.make_async_copy(ref, ref, recv.at[stage, k]).wait()

    def sent(ref, stage, k):
        pltpu.make_async_copy(ref, ref, send.at[stage, k]).wait()

    def aa_peers():
        for dx, dz, dc in AA_ORDER:
            xx, zz, cc = lax.rem(x + dx, 4), lax.rem(zh + dz, 2), lax.rem(c + dc, 2)
            yield cc * 8 + zz * 4 + xx, (zz, xx, cc, zl, y)

    def ba_peers():
        for dy, dz in BA_ORDER:
            yy, zz = lax.rem(y + dy, 4), lax.rem(zl + dz, 2)
            yield yy * 2 + zz, (zh, x, c, zz, yy)

    def xz_peers():
        for n, (dx, dz) in enumerate(XZ_ORDER):
            xx, zz = lax.rem(x + dx, 4), lax.rem(z + dz, 4)
            yield n, zz // 2 * 4 + xx, lax.rem(zz, 2), (zz // 2, xx, c, lax.rem(zz, 2), y)

    partner = (zh, x, 1 - c, zl, y)

    up = (zh, x, c, zl, lax.rem(y + 1, 4))
    down = (zh, x, c, zl, lax.rem(y + 3, 4))

    def meet():
        barrier = pltpu.get_barrier_semaphore()
        devices = [d for _, d in aa_peers()] + [d for _, d in ba_peers()]
        devices += [(zz // 2, xx, c, lax.rem(zz, 2), y) for xx, zz in
                    ((lax.rem(x + dx, 4), lax.rem(z + dz, 4)) for dx in range(4) for dz in (1, 3))]
        for device in devices:
            pl.semaphore_signal(barrier, inc=1, device_id=device, device_id_type=MESH)
        pl.semaphore_wait(barrier, len(devices))

    def tables():
        def rank_of(zz, xx, cc, zzl, yy):
            return depth[bricks[(((zz * 4 + xx) * 2 + cc) * 2 + zzl) * 4 + yy]]

        inner = [lax.rem(rank_of(r // 4 % 2, r % 4, r // 8, zl, y), 16) for r in range(16)]
        group = [lax.div(rank_of(zh, x, c, j % 2, j // 2), 16) for j in range(8)]

        def inverse(ranks, m):
            return functools.reduce(lambda a, iv: jnp.where(iv[1] == m, iv[0], a), enumerate(ranks), 0)

        return ([inverse(inner, m) for m in range(16)] + inner
                + [inverse(group, m) for m in range(8)] + group)

    def cols(k):
        return pl.ds(k * width, width)

    def own_alpha(k):
        return pltpu.make_async_copy(img.at[3, band, :, cols(k)], ain[k].at[band], own.at[0, k])

    def own_color(k):
        return pltpu.make_async_copy(img.at[pl.ds(0, 3), :, :, cols(k)], col.at[k], own.at[1, k])

    def alpha(k):
        for r, device in aa_peers():
            remote(img.at[3, r, :, cols(k)], ain[k].at[band], 0, k, device)
        own_alpha(k).start()

    def prefix(k):
        own_alpha(k).wait()
        arrived(ain[k].at[pl.ds(0, 15)], 0, k)
        run = jnp.ones((ROW, width), jnp.float32)
        for m in range(16):
            pre[k, m] = run
            run = run * (1.0 - ain[k][tab[m]])
        for j in range(8):
            gb[k, j] = run[:, j * tile:(j + 1) * tile]
        gin[k][slot_b] = gb[k, slot_b]
        for j, device in ba_peers():
            remote(gb.at[k, j], gin[k].at[slot_b], 1, k, device)

    def group(k):
        arrived(gin[k].at[pl.ds(0, 7)], 1, k)
        run = jnp.ones((ROW, tile), jnp.float32)
        for m in range(8):
            qb[k, m] = run
            run = run * gin[k][tab[32 + m]]
        out[3, band, :, pl.ds(pl.multiple_of(k * width + slot_b * tile, 128), tile)] = 1.0 - run
        for j in range(8):
            qout[k, j] = qb[k, tab[40 + j]]
        qin[k, slot_b] = qout[k, slot_b]
        for j, device in ba_peers():
            remote(qout.at[k, j], qin.at[k, slot_b], 2, k, device)

    def trans(k):
        arrived(qin.at[k, pl.ds(0, 7)], 2, k)
        q = jnp.concatenate([qin[k, j] for j in range(8)], axis=1)
        for r in range(16):
            tout[k, r] = pre[k, tab[16 + r]] * q
        tin[k, band] = tout[k, band]
        for r, device in aa_peers():
            remote(tout.at[k, r], tin.at[k, band], 3, k, device)

    def scale(k):
        own_color(k).wait()
        arrived(tin.at[k, pl.ds(0, 15)], 3, k)

        def body(i, carry):
            r = (1 - c) * 8 + i
            t = tin[k, r]
            for ch in range(3):
                cs[k, ch, i] = col[k, ch, r] * t
            return carry

        lax.fori_loop(0, 8, body, 0)
        remote(cs.at[k], cin.at[k], 4, k, partner)

    def sum_core(k):
        arrived(cin.at[k], 4, k)

        def body(i, carry):
            r = c * 8 + i
            t = tin[k, r]
            for ch in range(3):
                a1[k, ch, i] = col[k, ch, r] * t + cin[k, ch, i]
            return carry

        lax.fori_loop(0, 8, body, 0)
        def part(dy, half):
            q = pl.ds(pl.multiple_of(lax.rem(y + dy, 4) * quarter, 128), quarter)
            return a1.at[k, :, 4 * half:4 * half + 4, :, q]

        remote(part(2, 0), ys.at[k, 0], 5, k, up)
        remote(part(2, 1), ys.at[k, 1], 5, k, down)
        remote(part(1, 1), yin.at[k, 0, :, 4:8], 10, k, up)
        remote(part(3, 0), yin.at[k, 1, :, 0:4], 10, k, down)

    def around(k):
        arrived(ys.at[k], 5, k)
        for n, dy, device in ((0, 1, up), (1, 3, down)):
            q = pl.ds(pl.multiple_of(lax.rem(y + dy, 4) * quarter, 128), quarter)
            for ch in range(3):
                for i in range(4):
                    b1[k, n, ch, i] = a1[k, ch, 4 * n + i, :, q] + ys[k, n, ch, i]
            remote(b1.at[k, n], yin.at[k, n, :, 4 * n:4 * n + 4], 10, k, device)

    def sum_y(k):
        arrived(yin.at[k], 10, k)

        def body(i, carry):
            at = pl.ds(pl.multiple_of(y * quarter, 128), quarter)
            for ch in range(3):
                a2[k, ch, i] = a1[k, ch, i, :, at] + (yin[k, 0, ch, i] + yin[k, 1, ch, i])
            return carry

        lax.fori_loop(0, 8, body, 0)
        for n, r, t, device in xz_peers():
            at = pl.ds(pl.multiple_of(t * tile, 128), tile)
            remote(a2.at[k, :, r, :, at], xin.at[k, n], 6, k, device)

    def strip(k):
        return pl.ds(pl.multiple_of(k * width + slot_b * tile, 128), tile)

    def sum_xz(k):
        arrived(xin.at[k], 6, k)
        at = pl.ds(pl.multiple_of(zl * tile, 128), tile)
        for ch in range(3):
            s = a2[k, ch, zh * 4 + x, :, at]
            for n in range(15):
                s = s + xin[k, n, ch]
            out[ch, band, :, strip(k)] = s
        mine = out.at[:, band, :, strip(k)]
        for n, r, t, device in xz_peers():
            remote(mine, mine, 7, k, device)

    def piece(k, yy, cc):
        return out.at[:, pl.ds(pl.multiple_of(cc * 8, 8), 8), :, pl.ds(pl.multiple_of(k * width + yy * quarter, 128), quarter)]

    def gather_y(k):
        arrived(xin_like(k), 7, k)
        mine = piece(k, y, c)
        remote(mine, mine, 8, k, up)
        remote(mine, mine, 11, k, down)
        remote(mine, mine, 9, k, partner)

    def forward(k):
        whole = out.at[:, pl.ds(0, 8), :, pl.ds(0, quarter)]
        arrived(whole, 8, k)
        below = piece(k, lax.rem(y + 3, 4), c)
        remote(below.at[pl.ds(0, 2)], below.at[pl.ds(0, 2)], 12, k, up)
        remote(below, below, 9, k, partner)
        arrived(whole, 11, k)
        above = piece(k, lax.rem(y + 1, 4), c)
        remote(above.at[pl.ds(2, 2)], above.at[pl.ds(2, 2)], 12, k, down)
        remote(above, above, 9, k, partner)

    def xin_like(k):
        return out.at[:, pl.ds(0, 15), :, pl.ds(0, tile)]

    def gather_core(k):
        arrived(out.at[:, pl.ds(0, 8), :, pl.ds(0, quarter)], 12, k)
        far = piece(k, lax.rem(y + 2, 4), c)
        remote(far, far, 9, k, partner)

    def finish():
        whole = out.at[:, pl.ds(0, 8), :, pl.ds(0, quarter)]
        for k in range(CHUNKS):
            sent(ain[k].at[pl.ds(0, 15)], 0, k)
            sent(gb.at[k, pl.ds(0, 7)], 1, k)
            sent(qout.at[k, pl.ds(0, 7)], 2, k)
            sent(tout.at[k, pl.ds(0, 15)], 3, k)
            sent(cs.at[k], 4, k)
            sent(ys.at[k], 5, k)
            sent(yin.at[k], 10, k)
            sent(xin.at[k], 6, k)
            sent(xin_like(k), 7, k)
            sent(whole, 8, k)
            sent(whole, 11, k)
            sent(whole, 12, k)
            arrived(out.at[:, pl.ds(0, 8), :, pl.ds(0, width)], 9, k)
            sent(out.at[:, pl.ds(0, 8), :, pl.ds(0, width)], 9, k)

    def load():
        for k in range(CHUNKS):
            own_color(k).start()
        tab.extend(tables())

    tab = []
    stages = dict(alpha=alpha, prefix=prefix, group=group, trans=trans, scale=scale, sum_core=sum_core, around=around, sum_y=sum_y,
                  sum_xz=sum_xz, gather_y=gather_y, forward=forward, gather_core=gather_core)
    meet()
    for name in PLAN:
        with jax.named_scope(name):
            if name == "load":
                load()
            elif name == "finish":
                finish()
            else:
                stages[name[:-1]](int(name[-1]))


def local(images, depth, brick_map):
    channels, rows, columns = images.shape[1:]
    width = columns // CHUNKS
    tile, quarter = width // 8, width // 4
    f = jnp.float32
    n = CHUNKS
    vm = lambda *s: pltpu.VMEM(s, f)
    out = pl.pallas_call(
        kernel,
        out_shape=pltpu.VMEM((channels, rows // ROW, ROW, columns), f),
        in_specs=[pl.BlockSpec(memory_space=pltpu.SMEM), pl.BlockSpec(memory_space=pltpu.SMEM), pl.BlockSpec(memory_space=pl.ANY)],
        out_specs=pl.BlockSpec(memory_space=pltpu.VMEM),
        scratch_shapes=[
            *[vm(16, ROW, width)] * n, *[vm(8, ROW, tile)] * n,
            vm(n, 16, ROW, width), vm(n, 8, ROW, tile), vm(n, 8, ROW, tile), vm(n, 8, ROW, tile), vm(n, 8, ROW, tile),
            vm(n, 16, ROW, width), vm(n, 16, ROW, width),
            vm(n, 3, 16, ROW, width), vm(n, 3, 8, ROW, width), vm(n, 3, 8, ROW, width), vm(n, 3, 8, ROW, width),
            vm(n, 2, 3, 4, ROW, quarter), vm(n, 2, 3, 4, ROW, quarter), vm(n, 2, 3, 8, ROW, quarter), vm(n, 3, 8, ROW, quarter), vm(n, 15, 3, ROW, tile),
            pltpu.SemaphoreType.DMA((13, n)), pltpu.SemaphoreType.DMA((13, n)), pltpu.SemaphoreType.DMA((2, n)),
        ],
        compiler_params=pltpu.CompilerParams(has_side_effects=True, collective_id=0, vmem_limit_bytes=48 * 2**20),
    )(depth, brick_map, images.reshape(channels, rows // ROW, ROW, columns))
    return out.reshape(channels, rows, columns)


def solution(mesh):
    torus = Mesh(mesh.devices.reshape(2, 4, 2, 2, 4), AXES)
    return jax.shard_map(
        local,
        mesh=torus,
        in_specs=(P(("zh", "x", "c", "zl", "y"), None, None, None), P(), P()),
        out_specs=P(),
        check_vma=False,
    )
```

```python
import functools

import jax
import jax.numpy as jnp
from jax import lax
from jax.experimental import pallas as pl
from jax.experimental.pallas import tpu as pltpu
from jax.sharding import Mesh
from jax.sharding import PartitionSpec as P

AXES = ("zh", "x", "c", "zl", "y")
CHUNKS = 4
ROW = 8
MESH = pl.DeviceIdType.MESH

AA_ORDER = [(dx, dz, dc) for dc in (0, 1) for dx, dz in
            ((1, 1), (3, 1), (0, 1), (2, 1), (1, 0), (3, 0), (2, 0), (0, 0))][:]
AA_ORDER = [p for p in AA_ORDER if p != (0, 0, 0)]
BA_ORDER = [(dy, dz) for dy in (2, 1, 3, 0) for dz in (1, 0) if (dy, dz) != (0, 0)]
XZ_ORDER = [(dx, dz) for dx, dz in
            ((2, 2), (1, 2), (3, 2), (2, 1), (2, 3), (1, 1), (3, 3), (1, 3), (3, 1),
             (0, 2), (2, 0), (1, 0), (0, 1), (3, 0), (0, 3))]

PLAN = (
    "alpha0", "alpha1", "load", "prefix0", "alpha3", "prefix1", "group0", "alpha2", "prefix3", "group1",
    "trans0", "prefix2", "group3", "trans1", "scale0", "group2", "sum_core0", "trans3", "scale1", "around0",
    "sum_core1", "trans2", "scale3", "sum_y0", "around1", "sum_core3", "scale2", "sum_y1", "around3",
    "sum_core2", "sum_xz0", "sum_y3", "sum_xz1", "around2", "gather_y0", "sum_xz3", "sum_y2", "gather_y1",
    "gather_y3", "forward1", "forward0", "sum_xz2", "gather_y2", "gather_core1", "forward3", "forward2",
    "gather_core0", "gather_core3", "gather_core2", "finish",
)


def kernel(depth, bricks, img, out, *scratch):
    ain, gin = scratch[:CHUNKS], scratch[CHUNKS:2 * CHUNKS]
    pre, gb, qb, qout, qin, tout, tin, col, cs, cin, a1, ys, b1, yin, a2, xin, send, recv, own = scratch[2 * CHUNKS:]
    zh, x, c, zl, y = (lax.axis_index(a) for a in AXES)
    z = zh * 2 + zl
    width = tin.shape[-1]
    tile = width // 8
    quarter = width // 4
    band = c * 8 + zh * 4 + x
    slot_b = y * 2 + zl

    def remote(src, dst, stage, k, device):
        cp = pltpu.make_async_remote_copy(
            src_ref=src, dst_ref=dst, send_sem=send.at[stage, k], recv_sem=recv.at[stage, k],
            device_id=device, device_id_type=MESH)
        cp.start()

    def arrived(ref, stage, k):
        pltpu.make_async_copy(ref, ref, recv.at[stage, k]).wait()

    def sent(ref, stage, k):
        pltpu.make_async_copy(ref, ref, send.at[stage, k]).wait()

    def aa_peers():
        for dx, dz, dc in AA_ORDER:
            xx, zz, cc = lax.rem(x + dx, 4), lax.rem(zh + dz, 2), lax.rem(c + dc, 2)
            yield cc * 8 + zz * 4 + xx, (zz, xx, cc, zl, y)

    def ba_peers():
        for dy, dz in BA_ORDER:
            yy, zz = lax.rem(y + dy, 4), lax.rem(zl + dz, 2)
            yield yy * 2 + zz, (zh, x, c, zz, yy)

    def xz_peers():
        for n, (dx, dz) in enumerate(XZ_ORDER):
            xx, zz = lax.rem(x + dx, 4), lax.rem(z + dz, 4)
            yield n, zz // 2 * 4 + xx, lax.rem(zz, 2), (zz // 2, xx, c, lax.rem(zz, 2), y)

    partner = (zh, x, 1 - c, zl, y)

    up = (zh, x, c, zl, lax.rem(y + 1, 4))
    down = (zh, x, c, zl, lax.rem(y + 3, 4))

    def meet():
        barrier = pltpu.get_barrier_semaphore()
        devices = [d for _, d in aa_peers()] + [d for _, d in ba_peers()]
        devices += [(zz // 2, xx, c, lax.rem(zz, 2), y) for xx, zz in
                    ((lax.rem(x + dx, 4), lax.rem(z + dz, 4)) for dx in range(4) for dz in (1, 3))]
        for device in devices:
            pl.semaphore_signal(barrier, inc=1, device_id=device, device_id_type=MESH)
        pl.semaphore_wait(barrier, len(devices))

    def tables():
        def rank_of(zz, xx, cc, zzl, yy):
            return depth[bricks[(((zz * 4 + xx) * 2 + cc) * 2 + zzl) * 4 + yy]]

        inner = [lax.rem(rank_of(r // 4 % 2, r % 4, r // 8, zl, y), 16) for r in range(16)]
        group = [lax.div(rank_of(zh, x, c, j % 2, j // 2), 16) for j in range(8)]

        def inverse(ranks, m):
            return functools.reduce(lambda a, iv: jnp.where(iv[1] == m, iv[0], a), enumerate(ranks), 0)

        return ([inverse(inner, m) for m in range(16)] + inner
                + [inverse(group, m) for m in range(8)] + group)

    def cols(k):
        return pl.ds(k * width, width)

    def own_alpha(k):
        return pltpu.make_async_copy(img.at[3, band, :, cols(k)], ain[k].at[band], own.at[0, k])

    def own_color(k):
        return pltpu.make_async_copy(img.at[pl.ds(0, 3), :, :, cols(k)], col.at[k], own.at[1, k])

    def alpha(k, begin=0, end=15):
        for r, device in list(aa_peers())[begin:end]:
            remote(img.at[3, r, :, cols(k)], ain[k].at[band], 0, k, device)
        if begin == 0:
            own_alpha(k).start()

    def prefix(k):
        own_alpha(k).wait()
        arrived(ain[k].at[pl.ds(0, 15)], 0, k)
        run = jnp.ones((ROW, width), jnp.float32)
        for m in range(16):
            pre[k, m] = run
            run = run * (1.0 - ain[k][tab[m]])
        for j in range(8):
            gb[k, j] = run[:, j * tile:(j + 1) * tile]
        gin[k][slot_b] = gb[k, slot_b]
        for j, device in ba_peers():
            remote(gb.at[k, j], gin[k].at[slot_b], 1, k, device)

    def group(k):
        arrived(gin[k].at[pl.ds(0, 7)], 1, k)
        run = jnp.ones((ROW, tile), jnp.float32)
        for m in range(8):
            qb[k, m] = run
            run = run * gin[k][tab[32 + m]]
        out[3, band, :, pl.ds(pl.multiple_of(k * width + slot_b * tile, 128), tile)] = 1.0 - run
        for j in range(8):
            qout[k, j] = qb[k, tab[40 + j]]
        qin[k, slot_b] = qout[k, slot_b]
        for j, device in ba_peers():
            remote(qout.at[k, j], qin.at[k, slot_b], 2, k, device)

    def trans(k):
        arrived(qin.at[k, pl.ds(0, 7)], 2, k)
        q = jnp.concatenate([qin[k, j] for j in range(8)], axis=1)
        for r in range(16):
            tout[k, r] = pre[k, tab[16 + r]] * q
        tin[k, band] = tout[k, band]
        for r, device in aa_peers():
            remote(tout.at[k, r], tin.at[k, band], 3, k, device)

    def scale(k):
        own_color(k).wait()
        arrived(tin.at[k, pl.ds(0, 15)], 3, k)

        def body(i, carry):
            r = (1 - c) * 8 + i
            t = tin[k, r]
            for ch in range(3):
                cs[k, ch, i] = col[k, ch, r] * t
            return carry

        lax.fori_loop(0, 8, body, 0)
        remote(cs.at[k], cin.at[k], 4, k, partner)

    def sum_core(k):
        arrived(cin.at[k], 4, k)

        def body(i, carry):
            r = c * 8 + i
            t = tin[k, r]
            for ch in range(3):
                a1[k, ch, i] = col[k, ch, r] * t + cin[k, ch, i]
            return carry

        lax.fori_loop(0, 8, body, 0)
        def part(dy, half):
            q = pl.ds(pl.multiple_of(lax.rem(y + dy, 4) * quarter, 128), quarter)
            return a1.at[k, :, 4 * half:4 * half + 4, :, q]

        remote(part(2, 0), ys.at[k, 0], 5, k, up)
        remote(part(2, 1), ys.at[k, 1], 5, k, down)
        remote(part(1, 1), yin.at[k, 0, :, 4:8], 10, k, up)
        remote(part(3, 0), yin.at[k, 1, :, 0:4], 10, k, down)

    def around(k):
        arrived(ys.at[k], 5, k)
        for n, dy, device in ((0, 1, up), (1, 3, down)):
            q = pl.ds(pl.multiple_of(lax.rem(y + dy, 4) * quarter, 128), quarter)
            for ch in range(3):
                for i in range(4):
                    b1[k, n, ch, i] = a1[k, ch, 4 * n + i, :, q] + ys[k, n, ch, i]
            remote(b1.at[k, n], yin.at[k, n, :, 4 * n:4 * n + 4], 10, k, device)

    def sum_y(k):
        arrived(yin.at[k], 10, k)

        def body(i, carry):
            at = pl.ds(pl.multiple_of(y * quarter, 128), quarter)
            for ch in range(3):
                a2[k, ch, i] = a1[k, ch, i, :, at] + (yin[k, 0, ch, i] + yin[k, 1, ch, i])
            return carry

        lax.fori_loop(0, 8, body, 0)
        for n, r, t, device in xz_peers():
            at = pl.ds(pl.multiple_of(t * tile, 128), tile)
            remote(a2.at[k, :, r, :, at], xin.at[k, n], 6, k, device)

    def strip(k):
        return pl.ds(pl.multiple_of(k * width + slot_b * tile, 128), tile)

    def sum_xz(k):
        arrived(xin.at[k], 6, k)
        at = pl.ds(pl.multiple_of(zl * tile, 128), tile)
        for ch in range(3):
            s = a2[k, ch, zh * 4 + x, :, at]
            for n in range(15):
                s = s + xin[k, n, ch]
            out[ch, band, :, strip(k)] = s
        mine = out.at[:, band, :, strip(k)]
        for n, r, t, device in xz_peers():
            remote(mine, mine, 7, k, device)

    def piece(k, yy, cc):
        return out.at[:, pl.ds(pl.multiple_of(cc * 8, 8), 8), :, pl.ds(pl.multiple_of(k * width + yy * quarter, 128), quarter)]

    def gather_y(k):
        arrived(xin_like(k), 7, k)
        mine = piece(k, y, c)
        remote(mine, mine, 8, k, up)
        remote(mine, mine, 11, k, down)
        remote(mine, mine, 9, k, partner)

    def forward(k):
        whole = out.at[:, pl.ds(0, 8), :, pl.ds(0, quarter)]
        arrived(whole, 8, k)
        below = piece(k, lax.rem(y + 3, 4), c)
        remote(below.at[pl.ds(0, 2)], below.at[pl.ds(0, 2)], 12, k, up)
        remote(below, below, 9, k, partner)
        arrived(whole, 11, k)
        above = piece(k, lax.rem(y + 1, 4), c)
        remote(above.at[pl.ds(2, 2)], above.at[pl.ds(2, 2)], 12, k, down)
        remote(above, above, 9, k, partner)

    def xin_like(k):
        return out.at[:, pl.ds(0, 15), :, pl.ds(0, tile)]

    def gather_core(k):
        arrived(out.at[:, pl.ds(0, 8), :, pl.ds(0, quarter)], 12, k)
        far = piece(k, lax.rem(y + 2, 4), c)
        remote(far, far, 9, k, partner)

    def finish():
        whole = out.at[:, pl.ds(0, 8), :, pl.ds(0, quarter)]
        for k in range(CHUNKS):
            sent(ain[k].at[pl.ds(0, 15)], 0, k)
            sent(gb.at[k, pl.ds(0, 7)], 1, k)
            sent(qout.at[k, pl.ds(0, 7)], 2, k)
            sent(tout.at[k, pl.ds(0, 15)], 3, k)
            sent(cs.at[k], 4, k)
            sent(ys.at[k], 5, k)
            sent(yin.at[k], 10, k)
            sent(xin.at[k], 6, k)
            sent(xin_like(k), 7, k)
            sent(whole, 8, k)
            sent(whole, 11, k)
            sent(whole, 12, k)
            arrived(out.at[:, pl.ds(0, 8), :, pl.ds(0, width)], 9, k)
            sent(out.at[:, pl.ds(0, 8), :, pl.ds(0, width)], 9, k)

    def load():
        for k in range(CHUNKS):
            own_color(k).start()
        tab.extend(tables())

    tab = []
    stages = dict(alpha=alpha, prefix=prefix, group=group, trans=trans, scale=scale, sum_core=sum_core, around=around, sum_y=sum_y,
                  sum_xz=sum_xz, gather_y=gather_y, forward=forward, gather_core=gather_core)
    meet()
    for name in PLAN:
        with jax.named_scope(name):
            if name == "load":
                load()
            elif name == "finish":
                finish()
            elif name[-1] == "a":
                alpha(int(name[-2]), 0, 7)
            elif name[-1] == "b":
                alpha(int(name[-2]), 7, 15)
            else:
                stages[name[:-1]](int(name[-1]))


def local(images, depth, brick_map):
    channels, rows, columns = images.shape[1:]
    width = columns // CHUNKS
    tile, quarter = width // 8, width // 4
    f = jnp.float32
    n = CHUNKS
    vm = lambda *s: pltpu.VMEM(s, f)
    out = pl.pallas_call(
        kernel,
        out_shape=pltpu.VMEM((channels, rows // ROW, ROW, columns), f),
        in_specs=[pl.BlockSpec(memory_space=pltpu.SMEM), pl.BlockSpec(memory_space=pltpu.SMEM), pl.BlockSpec(memory_space=pl.ANY)],
        out_specs=pl.BlockSpec(memory_space=pltpu.VMEM),
        scratch_shapes=[
            *[vm(16, ROW, width)] * n, *[vm(8, ROW, tile)] * n,
            vm(n, 16, ROW, width), vm(n, 8, ROW, tile), vm(n, 8, ROW, tile), vm(n, 8, ROW, tile), vm(n, 8, ROW, tile),
            vm(n, 16, ROW, width), vm(n, 16, ROW, width),
            vm(n, 3, 16, ROW, width), vm(n, 3, 8, ROW, width), vm(n, 3, 8, ROW, width), vm(n, 3, 8, ROW, width),
            vm(n, 2, 3, 4, ROW, quarter), vm(n, 2, 3, 4, ROW, quarter), vm(n, 2, 3, 8, ROW, quarter), vm(n, 3, 8, ROW, quarter), vm(n, 15, 3, ROW, tile),
            pltpu.SemaphoreType.DMA((13, n)), pltpu.SemaphoreType.DMA((13, n)), pltpu.SemaphoreType.DMA((2, n)),
        ],
        compiler_params=pltpu.CompilerParams(has_side_effects=True, collective_id=0, vmem_limit_bytes=48 * 2**20),
    )(depth, brick_map, images.reshape(channels, rows // ROW, ROW, columns))
    return out.reshape(channels, rows, columns)


def solution(mesh):
    torus = Mesh(mesh.devices.reshape(2, 4, 2, 2, 4), AXES)
    return jax.shard_map(
        local,
        mesh=torus,
        in_specs=(P(("zh", "x", "c", "zl", "y"), None, None, None), P(), P()),
        out_specs=P(),
        check_vma=False,
    )
```

```python
import functools

import jax
import jax.numpy as jnp
from jax import lax
from jax.experimental import pallas as pl
from jax.experimental.pallas import tpu as pltpu
from jax.sharding import Mesh
from jax.sharding import PartitionSpec as P

AXES = ("zh", "x", "c", "zl", "y")
CHUNKS = 4
SHARE = (4, 3, 2, 2)
ROW = 8
MESH = pl.DeviceIdType.MESH

AA_ORDER = [(dx, dz, dc) for dc in (0, 1) for dx, dz in
            ((1, 1), (3, 1), (0, 1), (2, 1), (1, 0), (3, 0), (2, 0), (0, 0))][:]
AA_ORDER = [p for p in AA_ORDER if p != (0, 0, 0)]
BA_ORDER = [(dy, dz) for dy in (2, 1, 3, 0) for dz in (1, 0) if (dy, dz) != (0, 0)]
XZ_ORDER = [(dx, dz) for dx, dz in
            ((2, 2), (1, 2), (3, 2), (2, 1), (2, 3), (1, 1), (3, 3), (1, 3), (3, 1),
             (0, 2), (2, 0), (1, 0), (0, 1), (3, 0), (0, 3))]

PLAN = (
    "alpha0", "load", "alpha1", "prefix0", "alpha2", "group0", "prefix1", "alpha3", "group1", "prefix2",
    "trans0", "prefix3", "group2", "trans1", "scale0", "group3", "sum_core0", "trans2", "scale1", "around0",
    "sum_core1", "trans3", "scale2", "around1", "sum_core2", "sum_y1", "sum_y0", "scale3", "around2",
    "sum_core3", "sum_xz1", "sum_y2", "sum_xz0", "around3", "gather_y1", "sum_y3", "sum_xz2", "gather_y0",
    "spread1", "sum_xz3", "gather_y2", "spread2", "forward1", "gather_y3", "forward2", "spread3",
    "gather_core1", "spread_core1", "spread_core2", "forward0", "gather_core2", "forward3", "gather_core0",
    "spread_core3", "gather_core3", "finish",
)


def kernel(depth, bricks, img, out, *scratch):
    ain, gin = scratch[:CHUNKS], scratch[CHUNKS:2 * CHUNKS]
    pre, gb, qb, qout, qin, tout, tin, col, cs, cin, a1, ys, b1, yin, a2, xin, send, recv, own = scratch[2 * CHUNKS:]
    zh, x, c, zl, y = (lax.axis_index(a) for a in AXES)
    z = zh * 2 + zl
    width = tin.shape[-1]
    tile = width // 8
    half = width // 2
    band = c * 8 + zh * 4 + x
    slot_b = zl * 4 + y

    def remote(src, dst, stage, k, device):
        cp = pltpu.make_async_remote_copy(
            src_ref=src, dst_ref=dst, send_sem=send.at[stage, k], recv_sem=recv.at[stage, k],
            device_id=device, device_id_type=MESH)
        cp.start()

    def arrived(ref, stage, k):
        pltpu.make_async_copy(ref, ref, recv.at[stage, k]).wait()

    def sent(ref, stage, k):
        pltpu.make_async_copy(ref, ref, send.at[stage, k]).wait()

    def aa_peers():
        for dx, dz, dc in AA_ORDER:
            xx, zz, cc = lax.rem(x + dx, 4), lax.rem(zh + dz, 2), lax.rem(c + dc, 2)
            yield cc * 8 + zz * 4 + xx, (zz, xx, cc, zl, y)

    def ba_peers():
        for dy, dz in BA_ORDER:
            yy, zz = lax.rem(y + dy, 4), lax.rem(zl + dz, 2)
            yield zz * 4 + yy, (zh, x, c, zz, yy)

    def xz_peers():
        for n, (dx, dz) in enumerate(XZ_ORDER):
            xx, zz = lax.rem(x + dx, 4), lax.rem(z + dz, 4)
            yield n, zz // 2 * 4 + xx, lax.rem(zz, 2), (zz // 2, xx, c, lax.rem(zz, 2), y)

    partner = (zh, x, 1 - c, zl, y)

    up = (zh, x, c, zl, lax.rem(y + 1, 4))
    down = (zh, x, c, zl, lax.rem(y + 3, 4))

    def meet():
        barrier = pltpu.get_barrier_semaphore()
        devices = [d for _, d in aa_peers()] + [d for _, d in ba_peers()]
        devices += [(zz // 2, xx, c, lax.rem(zz, 2), y) for xx, zz in
                    ((lax.rem(x + dx, 4), lax.rem(z + dz, 4)) for dx in range(4) for dz in (1, 3))]
        for device in devices:
            pl.semaphore_signal(barrier, inc=1, device_id=device, device_id_type=MESH)
        pl.semaphore_wait(barrier, len(devices))

    def tables():
        def rank_of(zz, xx, cc, zzl, yy):
            return depth[bricks[(((zz * 4 + xx) * 2 + cc) * 2 + zzl) * 4 + yy]]

        inner = [lax.rem(rank_of(r // 4 % 2, r % 4, r // 8, zl, y), 16) for r in range(16)]
        group = [lax.div(rank_of(zh, x, c, j // 4, j % 4), 16) for j in range(8)]

        def inverse(ranks, m):
            return functools.reduce(lambda a, iv: jnp.where(iv[1] == m, iv[0], a), enumerate(ranks), 0)

        return ([inverse(inner, m) for m in range(16)] + inner
                + [inverse(group, m) for m in range(8)] + group)

    def cols(k):
        return pl.ds(k * width, width)

    def own_alpha(k):
        return pltpu.make_async_copy(img.at[3, band, :, cols(k)], ain[k].at[band], own.at[0, k])

    def own_color(k):
        return pltpu.make_async_copy(img.at[pl.ds(0, 3), :, :, cols(k)], col.at[k], own.at[1, k])

    def alpha(k, begin=0, end=15):
        for r, device in list(aa_peers())[begin:end]:
            remote(img.at[3, r, :, cols(k)], ain[k].at[band], 0, k, device)
        if begin == 0:
            own_alpha(k).start()

    def prefix(k):
        own_alpha(k).wait()
        arrived(ain[k].at[pl.ds(0, 15)], 0, k)
        run = jnp.ones((ROW, width), jnp.float32)
        for m in range(16):
            pre[k, m] = run
            run = run * (1.0 - ain[k][tab[m]])
        for j in range(8):
            gb[k, j] = run[:, j * tile:(j + 1) * tile]
        gin[k][slot_b] = gb[k, slot_b]
        for j, device in ba_peers():
            remote(gb.at[k, j], gin[k].at[slot_b], 1, k, device)

    def group(k):
        arrived(gin[k].at[pl.ds(0, 7)], 1, k)
        run = jnp.ones((ROW, tile), jnp.float32)
        for m in range(8):
            qb[k, m] = run
            run = run * gin[k][tab[32 + m]]
        out[3, band, :, pl.ds(pl.multiple_of(k * width + slot_b * tile, 128), tile)] = 1.0 - run
        for j in range(8):
            qout[k, j] = qb[k, tab[40 + j]]
        qin[k, slot_b] = qout[k, slot_b]
        for j, device in ba_peers():
            remote(qout.at[k, j], qin.at[k, slot_b], 2, k, device)

    def trans(k):
        arrived(qin.at[k, pl.ds(0, 7)], 2, k)
        q = jnp.concatenate([qin[k, j] for j in range(8)], axis=1)
        for r in range(16):
            tout[k, r] = pre[k, tab[16 + r]] * q
        tin[k, band] = tout[k, band]
        for r, device in aa_peers():
            remote(tout.at[k, r], tin.at[k, band], 3, k, device)

    def scale(k):
        own_color(k).wait()
        arrived(tin.at[k, pl.ds(0, 15)], 3, k)

        def body(i, carry):
            r = (1 - c) * 8 + i
            t = tin[k, r]
            for ch in range(3):
                cs[k, ch, i] = col[k, ch, r] * t
            return carry

        lax.fori_loop(0, 8, body, 0)
        remote(cs.at[k], cin.at[k], 4, k, partner)

    def sum_core(k):
        arrived(cin.at[k], 4, k)

        def body(i, carry):
            r = c * 8 + i
            t = tin[k, r]
            for ch in range(3):
                v = col[k, ch, r] * t + cin[k, ch, i]
                a1[k, ch, i, 0] = v[:, :half]
                a1[k, ch, i, 1] = v[:, half:]
            return carry

        lax.fori_loop(0, 8, body, 0)
        def part(dy, h):
            return a1.at[k, :, 4 * h:4 * h + 4, :, :, tiles(dy)]

        remote(part(2, 0), ys.at[k, 0], 5, k, up)
        remote(part(2, 1), ys.at[k, 1], 5, k, down)
        remote(part(1, 1), yin.at[k, 0, :, 4:8], 10, k, up)
        remote(part(3, 0), yin.at[k, 1, :, 0:4], 10, k, down)

    def tiles(dy):
        return pl.ds(pl.multiple_of(lax.rem(y + dy, 4) * tile, 128), tile)

    def around(k):
        arrived(ys.at[k], 5, k)
        for n, dy, device in ((0, 1, up), (1, 3, down)):
            for ch in range(3):
                for i in range(4):
                    b1[k, n, ch, i] = a1[k, ch, 4 * n + i, :, :, tiles(dy)] + ys[k, n, ch, i]
            remote(b1.at[k, n], yin.at[k, n, :, 4 * n:4 * n + 4], 10, k, device)

    def sum_y(k):
        arrived(yin.at[k], 10, k)

        def body(i, carry):
            for ch in range(3):
                a2[k, ch, i] = a1[k, ch, i, :, :, tiles(0)] + (yin[k, 0, ch, i] + yin[k, 1, ch, i])
            return carry

        lax.fori_loop(0, 8, body, 0)
        for n, r, t, device in xz_peers():
            remote(a2.at[k, :, r, t], xin.at[k, n], 6, k, device)

    def strip(k):
        return pl.ds(pl.multiple_of(k * width + slot_b * tile, 128), tile)

    def sum_xz(k):
        arrived(xin.at[k], 6, k)
        for ch in range(3):
            v = a2[k, ch, zh * 4 + x, zl]
            for n in range(15):
                v = v + xin[k, n, ch]
            out[ch, band, :, strip(k)] = v
        if SHARE[k] < 4:
            mine = out.at[SHARE[k]:4, band, :, strip(k)]
            for dy in (2, 1, 3):
                remote(mine, mine, 13, k, (zh, x, c, zl, lax.rem(y + dy, 4)))
        if SHARE[k] > 0:
            mine = out.at[0:SHARE[k], band, :, strip(k)]
            for n, r, t, device in xz_peers():
                remote(mine, mine, 7, k, device)

    def block(k, first, last, count, columns):
        return out.at[first:last, pl.ds(0, count), :, pl.ds(0, columns)]

    def piece(k, dy, h):
        at = pl.multiple_of(k * width + h * half + lax.rem(y + dy, 4) * tile, 128)
        return out.at[0:SHARE[k], pl.ds(pl.multiple_of(c * 8, 8), 8), :, pl.ds(at, tile)]

    def gather_y(k):
        arrived(block(k, 0, SHARE[k], 15, tile), 7, k)
        for h in range(2):
            mine = piece(k, 0, h)
            remote(mine, mine, 8, k, up)
            remote(mine, mine, 11, k, down)
            remote(mine, mine, 9, k, partner)

    def forward(k):
        arrived(block(k, 0, SHARE[k], 8, 2 * tile), 8, k)
        below = [piece(k, 3, h) for h in range(2)]
        remote(below[0], below[0], 12, k, up)
        arrived(block(k, 0, SHARE[k], 8, 2 * tile), 11, k)
        above = [piece(k, 1, h) for h in range(2)]
        remote(above[1], above[1], 12, k, down)
        for ref in below + above:
            remote(ref, ref, 9, k, partner)

    def gather_core(k):
        arrived(block(k, 0, SHARE[k], 8, 2 * tile), 12, k)
        for h in range(2):
            far = piece(k, 2, h)
            remote(far, far, 9, k, partner)

    def spread(k):
        arrived(block(k, SHARE[k], 4, 3, tile), 13, k)
        mine = out.at[SHARE[k]:4, band, :, pl.ds(pl.multiple_of(k * width + zl * half, 128), half)]
        for n, r, t, device in xz_peers():
            remote(mine, mine, 14, k, device)

    def spread_core(k):
        arrived(block(k, SHARE[k], 4, 15, half), 14, k)
        mine = out.at[SHARE[k]:4, pl.ds(pl.multiple_of(c * 8, 8), 8), :, cols(k)]
        remote(mine, mine, 15, k, partner)

    def finish():
        for k in range(CHUNKS):
            sent(ain[k].at[pl.ds(0, 15)], 0, k)
            sent(gb.at[k, pl.ds(0, 7)], 1, k)
            sent(qout.at[k, pl.ds(0, 7)], 2, k)
            sent(tout.at[k, pl.ds(0, 15)], 3, k)
            sent(cs.at[k], 4, k)
            sent(ys.at[k], 5, k)
            sent(yin.at[k], 10, k)
            sent(xin.at[k], 6, k)
        for k in range(CHUNKS):
            s = SHARE[k]
            if s > 0:
                sent(block(k, 0, s, 15, tile), 7, k)
                for stage in (8, 11, 12):
                    sent(block(k, 0, s, 8, 2 * tile), stage, k)
                arrived(block(k, 0, s, 8, width), 9, k)
                sent(block(k, 0, s, 8, width), 9, k)
            if s < 4:
                sent(block(k, s, 4, 3, tile), 13, k)
                sent(block(k, s, 4, 15, half), 14, k)
                arrived(block(k, s, 4, 8, width), 15, k)
                sent(block(k, s, 4, 8, width), 15, k)

    def load():
        for k in range(CHUNKS):
            own_color(k).start()
        tab.extend(tables())

    tab = []
    stages = dict(alpha=alpha, prefix=prefix, group=group, trans=trans, scale=scale, sum_core=sum_core, around=around, sum_y=sum_y,
                  sum_xz=sum_xz, gather_y=gather_y, forward=forward, gather_core=gather_core, spread=spread,
                  spread_core=spread_core)
    meet()
    for name in PLAN:
        with jax.named_scope(name):
            if name == "load":
                load()
            elif name == "finish":
                finish()
            elif name[-1] == "a":
                alpha(int(name[-2]), 0, 7)
            elif name[-1] == "b":
                alpha(int(name[-2]), 7, 15)
            else:
                stages[name[:-1]](int(name[-1]))


def local(images, depth, brick_map):
    channels, rows, columns = images.shape[1:]
    width = columns // CHUNKS
    tile, half = width // 8, width // 2
    f = jnp.float32
    n = CHUNKS
    vm = lambda *s: pltpu.VMEM(s, f)
    out = pl.pallas_call(
        kernel,
        out_shape=pltpu.VMEM((channels, rows // ROW, ROW, columns), f),
        in_specs=[pl.BlockSpec(memory_space=pltpu.SMEM), pl.BlockSpec(memory_space=pltpu.SMEM), pl.BlockSpec(memory_space=pl.ANY)],
        out_specs=pl.BlockSpec(memory_space=pltpu.VMEM),
        scratch_shapes=[
            *[vm(16, ROW, width)] * n, *[vm(8, ROW, tile)] * n,
            vm(n, 16, ROW, width), vm(n, 8, ROW, tile), vm(n, 8, ROW, tile), vm(n, 8, ROW, tile), vm(n, 8, ROW, tile),
            vm(n, 16, ROW, width), vm(n, 16, ROW, width),
            vm(n, 3, 16, ROW, width), vm(n, 3, 8, ROW, width), vm(n, 3, 8, ROW, width), vm(n, 3, 8, 2, ROW, half),
            vm(n, 2, 3, 4, 2, ROW, tile), vm(n, 2, 3, 4, 2, ROW, tile), vm(n, 2, 3, 8, 2, ROW, tile), vm(n, 3, 8, 2, ROW, tile), vm(n, 15, 3, ROW, tile),
            pltpu.SemaphoreType.DMA((16, n)), pltpu.SemaphoreType.DMA((16, n)), pltpu.SemaphoreType.DMA((2, n)),
        ],
        compiler_params=pltpu.CompilerParams(has_side_effects=True, collective_id=0, vmem_limit_bytes=48 * 2**20),
    )(depth, brick_map, images.reshape(channels, rows // ROW, ROW, columns))
    return out.reshape(channels, rows, columns)


def solution(mesh):
    torus = Mesh(mesh.devices.reshape(2, 4, 2, 2, 4), AXES)
    return jax.shard_map(
        local,
        mesh=torus,
        in_specs=(P(("zh", "x", "c", "zl", "y"), None, None, None), P(), P()),
        out_specs=P(),
        check_vma=False,
    )
```

```python
import functools

import jax
import jax.numpy as jnp
from jax import lax
from jax.experimental import pallas as pl
from jax.experimental.pallas import tpu as pltpu
from jax.sharding import Mesh
from jax.sharding import PartitionSpec as P

AXES = ("zh", "x", "c", "zl", "y")
CHUNKS = 4
SHARE = (4, 2, 2, 2)
ROW = 8
MESH = pl.DeviceIdType.MESH

AA_ORDER = [(0, 0, 1), (0, 1, 0), (0, 1, 1), (1, 0, 0), (3, 1, 0), (2, 0, 0), (1, 1, 0), (3, 0, 0), (2, 1, 0),
            (1, 0, 1), (3, 1, 1), (2, 0, 1), (1, 1, 1), (3, 0, 1), (2, 1, 1)]
BA_ORDER = [(dy, dz) for dy in (2, 1, 3, 0) for dz in (1, 0) if (dy, dz) != (0, 0)]
XZ_ORDER = [(dx, dz) for dx, dz in
            ((2, 2), (1, 2), (3, 2), (2, 1), (2, 3), (1, 1), (3, 3), (1, 3), (3, 1),
             (0, 2), (2, 0), (1, 0), (0, 1), (3, 0), (0, 3))]

PLAN = (
    "alpha0", "load", "alpha1", "prefix0", "alpha2", "group0", "prefix1", "alpha3", "group1", "prefix2",
    "trans0", "prefix3", "group2", "trans1", "scale0", "group3", "sum_core0", "trans2", "scale1", "around0",
    "sum_core1", "trans3", "scale2", "around1", "sum_y0", "sum_core2", "scale3", "around2", "sum_y1",
    "sum_core3", "sum_xz0", "sum_xz1", "around3", "sum_y2", "gather_y0", "spread1", "sum_y3", "sum_xz2",
    "gather_y1", "cross1", "sum_xz3", "forward0", "gather_y2", "spread2", "spread3", "spread_core1", "cross2",
    "gather_y3", "gather_core0", "forward1", "cross3", "forward2", "spread_core2", "forward3", "gather_core1",
    "spread_core3", "gather_core2", "gather_core3", "finish",
)


def kernel(depth, bricks, img, out, *scratch):
    ain, gin = scratch[:CHUNKS], scratch[CHUNKS:2 * CHUNKS]
    pre, gb, qb, qout, qin, tout, tin, col, cs, cin, a1, ys, b1, yin, a2, xin, send, recv, own = scratch[2 * CHUNKS:]
    zh, x, c, zl, y = (lax.axis_index(a) for a in AXES)
    z = zh * 2 + zl
    width = tin.shape[-1]
    tile = width // 8
    half = width // 2
    band = c * 8 + zh * 4 + x
    slot_b = zl * 4 + y

    def remote(src, dst, stage, k, device):
        cp = pltpu.make_async_remote_copy(
            src_ref=src, dst_ref=dst, send_sem=send.at[stage, k], recv_sem=recv.at[stage, k],
            device_id=device, device_id_type=MESH)
        cp.start()

    def arrived(ref, stage, k):
        pltpu.make_async_copy(ref, ref, recv.at[stage, k]).wait()

    def sent(ref, stage, k):
        pltpu.make_async_copy(ref, ref, send.at[stage, k]).wait()

    def aa_peers():
        for dx, dz, dc in AA_ORDER:
            xx, zz, cc = lax.rem(x + dx, 4), lax.rem(zh + dz, 2), lax.rem(c + dc, 2)
            yield cc * 8 + zz * 4 + xx, (zz, xx, cc, zl, y)

    def ba_peers():
        for dy, dz in BA_ORDER:
            yy, zz = lax.rem(y + dy, 4), lax.rem(zl + dz, 2)
            yield zz * 4 + yy, (zh, x, c, zz, yy)

    def xz_peers():
        for n, (dx, dz) in enumerate(XZ_ORDER):
            xx, zz = lax.rem(x + dx, 4), lax.rem(z + dz, 4)
            yield n, zz // 2 * 4 + xx, lax.rem(zz, 2), (zz // 2, xx, c, lax.rem(zz, 2), y)

    partner = (zh, x, 1 - c, zl, y)

    up = (zh, x, c, zl, lax.rem(y + 1, 4))
    down = (zh, x, c, zl, lax.rem(y + 3, 4))

    def meet():
        barrier = pltpu.get_barrier_semaphore()
        devices = [d for _, d in aa_peers()] + [d for _, d in ba_peers()]
        devices += [(zz // 2, xx, c, lax.rem(zz, 2), y) for xx, zz in
                    ((lax.rem(x + dx, 4), lax.rem(z + dz, 4)) for dx in range(4) for dz in (1, 3))]
        for device in devices:
            pl.semaphore_signal(barrier, inc=1, device_id=device, device_id_type=MESH)
        pl.semaphore_wait(barrier, len(devices))

    def tables():
        def rank_of(zz, xx, cc, zzl, yy):
            return depth[bricks[(((zz * 4 + xx) * 2 + cc) * 2 + zzl) * 4 + yy]]

        inner = [lax.rem(rank_of(r // 4 % 2, r % 4, r // 8, zl, y), 16) for r in range(16)]
        group = [lax.div(rank_of(zh, x, c, j // 4, j % 4), 16) for j in range(8)]

        def inverse(ranks, m):
            return functools.reduce(lambda a, iv: jnp.where(iv[1] == m, iv[0], a), enumerate(ranks), 0)

        return ([inverse(inner, m) for m in range(16)] + inner
                + [inverse(group, m) for m in range(8)] + group)

    def cols(k):
        return pl.ds(k * width, width)

    def own_alpha(k):
        return pltpu.make_async_copy(img.at[3, c, zh, x, :, cols(k)], ain[k].at[band], own.at[0, k])

    def own_color(k):
        return pltpu.make_async_copy(img.at[0:3, :, :, :, :, cols(k)], col.at[k], own.at[1, k])

    def alpha(k, begin=0, end=15):
        for (zz, xx, cc, _, _), device in [(d, d) for _, d in aa_peers()][begin:end]:
            remote(img.at[3, cc, zz, xx, :, cols(k)], ain[k].at[band], 0, k, device)
        if begin == 0:
            own_alpha(k).start()

    def prefix(k):
        own_alpha(k).wait()
        arrived(ain[k].at[pl.ds(0, 15)], 0, k)
        run = jnp.ones((ROW, width), jnp.float32)
        for m in range(16):
            pre[k, m] = run
            run = run * (1.0 - ain[k][tab[m]])
        for j in range(8):
            gb[k, j] = run[:, j * tile:(j + 1) * tile]
        gin[k][slot_b] = gb[k, slot_b]
        for j, device in ba_peers():
            remote(gb.at[k, j], gin[k].at[slot_b], 1, k, device)

    def group(k):
        arrived(gin[k].at[pl.ds(0, 7)], 1, k)
        run = jnp.ones((ROW, tile), jnp.float32)
        for m in range(8):
            qb[k, m] = run
            run = run * gin[k][tab[32 + m]]
        out[3, c, zh, x, :, strip(k)] = 1.0 - run
        for j in range(8):
            qout[k, j] = qb[k, tab[40 + j]]
        qin[k, slot_b] = qout[k, slot_b]
        for j, device in ba_peers():
            remote(qout.at[k, j], qin.at[k, slot_b], 2, k, device)

    def trans(k):
        arrived(qin.at[k, pl.ds(0, 7)], 2, k)
        q = jnp.concatenate([qin[k, j] for j in range(8)], axis=1)
        for r in range(16):
            tout[k, r] = pre[k, tab[16 + r]] * q
        tin[k, band] = tout[k, band]
        for r, device in aa_peers():
            remote(tout.at[k, r], tin.at[k, band], 3, k, device)

    def scale(k):
        own_color(k).wait()
        arrived(tin.at[k, pl.ds(0, 15)], 3, k)

        def body(i, carry):
            r = (1 - c) * 8 + i
            t = tin[k, r]
            for ch in range(3):
                cs[k, ch, i] = col[k, ch, 1 - c, i // 4, i % 4] * t
            return carry

        lax.fori_loop(0, 8, body, 0)
        remote(cs.at[k], cin.at[k], 4, k, partner)

    def sum_core(k):
        arrived(cin.at[k], 4, k)

        def body(i, carry):
            r = c * 8 + i
            t = tin[k, r]
            for ch in range(3):
                v = col[k, ch, c, i // 4, i % 4] * t + cin[k, ch, i]
                a1[k, ch, i, 0] = v[:, :half]
                a1[k, ch, i, 1] = v[:, half:]
            return carry

        lax.fori_loop(0, 8, body, 0)
        def part(dy, h):
            return a1.at[k, :, 4 * h:4 * h + 4, :, :, tiles(dy)]

        remote(part(2, 0), ys.at[k, 0], 5, k, up)
        remote(part(2, 1), ys.at[k, 1], 5, k, down)
        remote(part(1, 1), yin.at[k, 0, :, 4:8], 10, k, up)
        remote(part(3, 0), yin.at[k, 1, :, 0:4], 10, k, down)

    def tiles(dy):
        return pl.ds(pl.multiple_of(lax.rem(y + dy, 4) * tile, 128), tile)

    def around(k):
        arrived(ys.at[k], 5, k)
        for n, dy, device in ((0, 1, up), (1, 3, down)):
            for ch in range(3):
                for i in range(4):
                    b1[k, n, ch, i] = a1[k, ch, 4 * n + i, :, :, tiles(dy)] + ys[k, n, ch, i]
            remote(b1.at[k, n], yin.at[k, n, :, 4 * n:4 * n + 4], 10, k, device)

    def sum_y(k):
        arrived(yin.at[k], 10, k)

        def body(i, carry):
            for ch in range(3):
                a2[k, ch, i] = a1[k, ch, i, :, :, tiles(0)] + (yin[k, 0, ch, i] + yin[k, 1, ch, i])
            return carry

        lax.fori_loop(0, 8, body, 0)
        for n, r, t, device in xz_peers():
            remote(a2.at[k, :, r, t], xin.at[k, n], 6, k, device)

    def strip(k):
        return pl.ds(pl.multiple_of(k * width + slot_b * tile, 128), tile)

    def sum_xz(k):
        arrived(xin.at[k], 6, k)
        for ch in range(3):
            v = a2[k, ch, zh * 4 + x, zl]
            for n in range(15):
                v = v + xin[k, n, ch]
            out[ch, c, zh, x, :, strip(k)] = v
        if SHARE[k] < 4:
            mine = out.at[SHARE[k]:4, c, zh, x, :, strip(k)]
            for dy in (2, 1, 3):
                remote(mine, mine, 13, k, (zh, x, c, zl, lax.rem(y + dy, 4)))
        if SHARE[k] > 0:
            mine = out.at[0:SHARE[k], c, zh, x, :, strip(k)]
            for n, r, t, device in xz_peers():
                remote(mine, mine, 7, k, device)

    def block(k, first, last, count, columns):
        return pre.at[0:last - first, 0:count, :, 0:columns]

    def piece(k, dy, h):
        at = pl.multiple_of(k * width + h * half + lax.rem(y + dy, 4) * tile, 128)
        return out.at[0:SHARE[k], c, :, :, :, pl.ds(at, tile)]

    def gather_y(k):
        arrived(block(k, 0, SHARE[k], 15, tile), 7, k)
        for h in range(2):
            mine = piece(k, 0, h)
            remote(mine, mine, 8, k, up)
            remote(mine, mine, 11, k, down)
            remote(mine, mine, 9, k, partner)

    def forward(k):
        arrived(block(k, 0, SHARE[k], 8, 2 * tile), 8, k)
        below = [piece(k, 3, h) for h in range(2)]
        remote(below[0], below[0], 12, k, up)
        arrived(block(k, 0, SHARE[k], 8, 2 * tile), 11, k)
        above = [piece(k, 1, h) for h in range(2)]
        remote(above[1], above[1], 12, k, down)
        for ref in below + above:
            remote(ref, ref, 9, k, partner)

    def gather_core(k):
        arrived(block(k, 0, SHARE[k], 8, 2 * tile), 12, k)
        for h in range(2):
            far = piece(k, 2, h)
            remote(far, far, 9, k, partner)

    def spread(k):
        arrived(block(k, SHARE[k], 4, 3, tile), 13, k)
        for h in range(2):
            mine = out.at[SHARE[k]:4, c, zh, x, :, columns(k, zl, h)]
            for n in (2, 1, 3):
                zz = lax.rem(z + n, 4)
                device = (zz // 2, x, c, lax.rem(zz, 2), y) if h else (zh, lax.rem(x + n, 4), c, zl, y)
                remote(mine, mine, 16 if h else 14, k, device)

    def columns(k, zzl, h):
        return pl.ds(pl.multiple_of(k * width + zzl * half + h * (half // 2), 128), half // 2)

    def cross(k):
        arrived(block(k, SHARE[k], 4, 3, half // 2), 14, k)
        row = out.at[SHARE[k]:4, c, zh, :, :, columns(k, zl, 0)]
        for n in (2, 1, 3):
            zz = lax.rem(z + n, 4)
            remote(row, row, 17, k, (zz // 2, x, c, lax.rem(zz, 2), y))
        arrived(block(k, SHARE[k], 4, 3, half // 2), 16, k)
        for n in (2, 1, 3):
            for h in range(2):
                line = out.at[SHARE[k]:4, c, :, x, :, columns(k, h, 1)]
                remote(line, line, 17, k, (zh, lax.rem(x + n, 4), c, zl, y))

    def spread_core(k):
        arrived(block(k, SHARE[k], 4, 12, half), 17, k)
        mine = out.at[SHARE[k]:4, c, :, :, :, cols(k)]
        remote(mine, mine, 15, k, partner)

    def finish():
        for k in range(CHUNKS):
            sent(ain[k].at[pl.ds(0, 15)], 0, k)
            sent(gb.at[k, pl.ds(0, 7)], 1, k)
            sent(qout.at[k, pl.ds(0, 7)], 2, k)
            sent(tout.at[k, pl.ds(0, 15)], 3, k)
            sent(cs.at[k], 4, k)
            sent(ys.at[k], 5, k)
            sent(yin.at[k], 10, k)
            sent(xin.at[k], 6, k)
        for k in range(CHUNKS):
            s = SHARE[k]
            if s > 0:
                sent(block(k, 0, s, 15, tile), 7, k)
                for stage in (8, 11, 12):
                    sent(block(k, 0, s, 8, 2 * tile), stage, k)
                arrived(block(k, 0, s, 8, width), 9, k)
                sent(block(k, 0, s, 8, width), 9, k)
            if s < 4:
                sent(block(k, s, 4, 3, tile), 13, k)
                sent(block(k, s, 4, 3, half // 2), 14, k)
                sent(block(k, s, 4, 3, half // 2), 16, k)
                sent(block(k, s, 4, 12, half), 17, k)
                arrived(block(k, s, 4, 8, width), 15, k)
                sent(block(k, s, 4, 8, width), 15, k)

    def load():
        for k in range(CHUNKS):
            own_color(k).start()
        tab.extend(tables())

    tab = []
    stages = dict(alpha=alpha, prefix=prefix, group=group, trans=trans, scale=scale, sum_core=sum_core, around=around, sum_y=sum_y,
                  sum_xz=sum_xz, gather_y=gather_y, forward=forward, gather_core=gather_core, spread=spread, cross=cross,
                  spread_core=spread_core)
    meet()
    for name in PLAN:
        with jax.named_scope(name):
            if name == "load":
                load()
            elif name == "finish":
                finish()
            elif name[-1] == "a":
                alpha(int(name[-2]), 0, 7)
            elif name[-1] == "b":
                alpha(int(name[-2]), 7, 15)
            else:
                stages[name[:-1]](int(name[-1]))


def local(images, depth, brick_map):
    channels, rows, columns = images.shape[1:]
    width = columns // CHUNKS
    tile, half = width // 8, width // 2
    f = jnp.float32
    n = CHUNKS
    vm = lambda *s: pltpu.VMEM(s, f)
    out = pl.pallas_call(
        kernel,
        out_shape=pltpu.VMEM((channels, 2, 2, 4, ROW, columns), f),
        in_specs=[pl.BlockSpec(memory_space=pltpu.SMEM), pl.BlockSpec(memory_space=pltpu.SMEM), pl.BlockSpec(memory_space=pl.ANY)],
        out_specs=pl.BlockSpec(memory_space=pltpu.VMEM),
        scratch_shapes=[
            *[vm(16, ROW, width)] * n, *[vm(8, ROW, tile)] * n,
            vm(n, 16, ROW, width), vm(n, 8, ROW, tile), vm(n, 8, ROW, tile), vm(n, 8, ROW, tile), vm(n, 8, ROW, tile),
            vm(n, 16, ROW, width), vm(n, 16, ROW, width),
            vm(n, 3, 2, 2, 4, ROW, width), vm(n, 3, 8, ROW, width), vm(n, 3, 8, ROW, width), vm(n, 3, 8, 2, ROW, half),
            vm(n, 2, 3, 4, 2, ROW, tile), vm(n, 2, 3, 4, 2, ROW, tile), vm(n, 2, 3, 8, 2, ROW, tile), vm(n, 3, 8, 2, ROW, tile), vm(n, 15, 3, ROW, tile),
            pltpu.SemaphoreType.DMA((18, n)), pltpu.SemaphoreType.DMA((18, n)), pltpu.SemaphoreType.DMA((2, n)),
        ],
        compiler_params=pltpu.CompilerParams(has_side_effects=True, collective_id=0, vmem_limit_bytes=48 * 2**20),
    )(depth, brick_map, images.reshape(channels, 2, 2, 4, ROW, columns))
    return out.reshape(channels, rows, columns)


def solution(mesh):
    torus = Mesh(mesh.devices.reshape(2, 4, 2, 2, 4), AXES)
    return jax.shard_map(
        local,
        mesh=torus,
        in_specs=(P(("zh", "x", "c", "zl", "y"), None, None, None), P(), P()),
        out_specs=P(),
        check_vma=False,
    )
```

```python
import functools
import itertools
import math

import jax
import jax.numpy as jnp
from jax import lax
from jax.experimental import pallas as pl
from jax.experimental.pallas import tpu as pltpu
from jax.sharding import Mesh
from jax.sharding import PartitionSpec as P

AXES = ("zh", "x", "c", "zl", "y")
CHUNKS = 4
SHARE = (4, 2, 2, 2)
ROW = 8
MESH = pl.DeviceIdType.MESH

AA_ORDER = [(0, 0, 1), (0, 1, 0), (0, 1, 1), (1, 0, 0), (3, 1, 0), (2, 0, 0), (1, 1, 0), (3, 0, 0), (2, 1, 0),
            (1, 0, 1), (3, 1, 1), (2, 0, 1), (1, 1, 1), (3, 0, 1), (2, 1, 1)]
BA_ORDER = [(dy, dz) for dy in (2, 1, 3, 0) for dz in (1, 0) if (dy, dz) != (0, 0)]
XZ_ORDER = [(dx, dz) for dx, dz in
            ((2, 2), (1, 2), (3, 2), (2, 1), (2, 3), (1, 1), (3, 3), (1, 3), (3, 1),
             (0, 2), (2, 0), (1, 0), (0, 1), (3, 0), (0, 3))]

PLAN = (
    "alpha0", "load", "alpha1", "prefix0", "alpha2", "group0", "prefix1", "alpha3", "group1", "prefix2",
    "trans0", "prefix3", "group2", "trans1", "scale0", "group3", "sum_core0", "trans2", "scale1", "around0",
    "sum_core1", "trans3", "scale2", "around1", "sum_y0", "sum_core2", "scale3", "around2", "sum_y1",
    "sum_core3", "sum_xz0", "sum_xz1", "around3", "sum_y2", "gather_y0", "spread1", "sum_y3", "sum_xz2",
    "gather_y1", "cross1", "sum_xz3", "forward0", "gather_y2", "spread2", "spread3", "spread_core1", "cross2",
    "gather_y3", "gather_core0", "forward1", "cross3", "forward2", "spread_core2", "forward3", "gather_core1",
    "spread_core3", "gather_core2", "gather_core3", "finish",
)


def kernel(depth_in, bricks_in, img, out, *scratch):
    ain, gin = scratch[:CHUNKS], scratch[CHUNKS:2 * CHUNKS]
    pre, gb, qb, qout, qin, tout, tin, col, cs, cin, a1, ys, b1, yin, a2, xin, send, recv, own, depth, bricks = scratch[2 * CHUNKS:]
    zh, x, c, zl, y = (lax.axis_index(a) for a in AXES)
    z = zh * 2 + zl
    width = tin.shape[-1]
    tile = width // 8
    half = width // 2
    band = c * 8 + zh * 4 + x
    slot_b = zl * 4 + y

    def remote(src, dst, stage, k, device):
        cp = pltpu.make_async_remote_copy(
            src_ref=src, dst_ref=dst, send_sem=send.at[stage], recv_sem=recv.at[stage, k],
            device_id=device, device_id_type=MESH)
        cp.start()

    def arrived(ref, stage, k):
        pltpu.make_async_copy(ref, ref, recv.at[stage, k]).wait()

    def aa_peers():
        for dx, dz, dc in AA_ORDER:
            xx, zz, cc = lax.rem(x + dx, 4), lax.rem(zh + dz, 2), lax.rem(c + dc, 2)
            yield cc * 8 + zz * 4 + xx, (zz, xx, cc, zl, y)

    def ba_peers():
        for dy, dz in BA_ORDER:
            yy, zz = lax.rem(y + dy, 4), lax.rem(zl + dz, 2)
            yield zz * 4 + yy, (zh, x, c, zz, yy)

    def xz_peers():
        for n, (dx, dz) in enumerate(XZ_ORDER):
            xx, zz = lax.rem(x + dx, 4), lax.rem(z + dz, 4)
            yield n, zz // 2 * 4 + xx, lax.rem(zz, 2), (zz // 2, xx, c, lax.rem(zz, 2), y)

    partner = (zh, x, 1 - c, zl, y)

    up = (zh, x, c, zl, lax.rem(y + 1, 4))
    down = (zh, x, c, zl, lax.rem(y + 3, 4))

    def meet():
        barrier = pltpu.get_barrier_semaphore()
        devices = [d for _, d in aa_peers()] + [d for _, d in ba_peers()]
        devices += [(zz // 2, xx, c, lax.rem(zz, 2), y) for xx, zz in
                    ((lax.rem(x + dx, 4), lax.rem(z + dz, 4)) for dx in range(4) for dz in (1, 3))]
        for device in devices:
            pl.semaphore_signal(barrier, inc=1, device_id=device, device_id_type=MESH)
        pl.semaphore_wait(barrier, len(devices))

    def tables():
        def rank_of(zz, xx, cc, zzl, yy):
            return depth[bricks[(((zz * 4 + xx) * 2 + cc) * 2 + zzl) * 4 + yy]]

        inner = [lax.rem(rank_of(r // 4 % 2, r % 4, r // 8, zl, y), 16) for r in range(16)]
        group = [lax.div(rank_of(zh, x, c, j // 4, j % 4), 16) for j in range(8)]

        def inverse(ranks, m):
            return functools.reduce(lambda a, iv: jnp.where(iv[1] == m, iv[0], a), enumerate(ranks), 0)

        return ([inverse(inner, m) for m in range(16)] + inner
                + [inverse(group, m) for m in range(8)] + group)

    def cols(k):
        return pl.ds(k * width, width)

    def own_alpha(k):
        return pltpu.make_async_copy(img.at[3, c, zh, x, :, cols(k)], ain[k].at[band], own.at[0, k])

    def own_color(k):
        return pltpu.make_async_copy(img.at[0:3, :, :, :, :, cols(k)], col.at[k], own.at[1, k])

    def alpha(k, begin=0, end=15):
        for (zz, xx, cc, _, _), device in [(d, d) for _, d in aa_peers()][begin:end]:
            remote(img.at[3, cc, zz, xx, :, cols(k)], ain[k].at[band], 0, k, device)
        if begin == 0:
            own_alpha(k).start()

    def prefix(k):
        own_alpha(k).wait()
        arrived(ain[k].at[pl.ds(0, 15)], 0, k)
        run = jnp.ones((ROW, width), jnp.float32)
        for m in range(16):
            pre[k, m] = run
            run = run * (1.0 - ain[k][tab[m]])
        for j in range(8):
            gb[k, j] = run[:, j * tile:(j + 1) * tile]
        gin[k][slot_b] = gb[k, slot_b]
        for j, device in ba_peers():
            remote(gb.at[k, j], gin[k].at[slot_b], 1, k, device)

    def group(k):
        arrived(gin[k].at[pl.ds(0, 7)], 1, k)
        run = jnp.ones((ROW, tile), jnp.float32)
        for m in range(8):
            qb[k, m] = run
            run = run * gin[k][tab[32 + m]]
        out[3, c, zh, x, :, strip(k)] = 1.0 - run
        for j in range(8):
            qout[k, j] = qb[k, tab[40 + j]]
        qin[k, slot_b] = qout[k, slot_b]
        for j, device in ba_peers():
            remote(qout.at[k, j], qin.at[k, slot_b], 2, k, device)

    def trans(k):
        arrived(qin.at[k, pl.ds(0, 7)], 2, k)
        q = jnp.concatenate([qin[k, j] for j in range(8)], axis=1)
        for r in range(16):
            tout[k, r] = pre[k, tab[16 + r]] * q
        tin[k, band] = tout[k, band]
        for r, device in aa_peers():
            remote(tout.at[k, r], tin.at[k, band], 3, k, device)

    def scale(k):
        own_color(k).wait()
        arrived(tin.at[k, pl.ds(0, 15)], 3, k)

        def body(i, carry):
            r = (1 - c) * 8 + i
            t = tin[k, r]
            for ch in range(3):
                cs[k, ch, i] = col[k, ch, 1 - c, i // 4, i % 4] * t
            return carry

        lax.fori_loop(0, 8, body, 0)
        remote(cs.at[k], cin.at[k], 4, k, partner)

    def sum_core(k):
        arrived(cin.at[k], 4, k)

        def body(i, carry):
            r = c * 8 + i
            t = tin[k, r]
            for ch in range(3):
                v = col[k, ch, c, i // 4, i % 4] * t + cin[k, ch, i]
                a1[k, ch, i, 0] = v[:, :half]
                a1[k, ch, i, 1] = v[:, half:]
            return carry

        lax.fori_loop(0, 8, body, 0)
        def part(dy, h):
            return a1.at[k, :, 4 * h:4 * h + 4, :, :, tiles(dy)]

        remote(part(2, 0), ys.at[k, 0], 5, k, up)
        remote(part(2, 1), ys.at[k, 1], 5, k, down)
        remote(part(1, 1), yin.at[k, 0, :, 4:8], 10, k, up)
        remote(part(3, 0), yin.at[k, 1, :, 0:4], 10, k, down)

    def tiles(dy):
        return pl.ds(pl.multiple_of(lax.rem(y + dy, 4) * tile, 128), tile)

    def around(k):
        arrived(ys.at[k], 5, k)
        for n, dy, device in ((0, 1, up), (1, 3, down)):
            for ch in range(3):
                for i in range(4):
                    b1[k, n, ch, i] = a1[k, ch, 4 * n + i, :, :, tiles(dy)] + ys[k, n, ch, i]
            remote(b1.at[k, n], yin.at[k, n, :, 4 * n:4 * n + 4], 10, k, device)

    def sum_y(k):
        arrived(yin.at[k], 10, k)

        def body(i, carry):
            for ch in range(3):
                a2[k, ch, i] = a1[k, ch, i, :, :, tiles(0)] + (yin[k, 0, ch, i] + yin[k, 1, ch, i])
            return carry

        lax.fori_loop(0, 8, body, 0)
        for n, r, t, device in xz_peers():
            remote(a2.at[k, :, r, t], xin.at[k, n], 6, k, device)

    def strip(k):
        return pl.ds(pl.multiple_of(k * width + slot_b * tile, 128), tile)

    def sum_xz(k):
        arrived(xin.at[k], 6, k)
        for ch in range(3):
            v = a2[k, ch, zh * 4 + x, zl]
            for n in range(15):
                v = v + xin[k, n, ch]
            out[ch, c, zh, x, :, strip(k)] = v
        if SHARE[k] < 4:
            mine = out.at[SHARE[k]:4, c, zh, x, :, strip(k)]
            for dy in (2, 1, 3):
                remote(mine, mine, 13, k, (zh, x, c, zl, lax.rem(y + dy, 4)))
        if SHARE[k] > 0:
            mine = out.at[0:SHARE[k], c, zh, x, :, strip(k)]
            for n, r, t, device in xz_peers():
                remote(mine, mine, 7, k, device)

    def block(k, first, last, count, columns):
        return pre.at[0:last - first, 0:count, :, 0:columns]

    def piece(k, dy, h):
        at = pl.multiple_of(k * width + h * half + lax.rem(y + dy, 4) * tile, 128)
        return out.at[0:SHARE[k], c, :, :, :, pl.ds(at, tile)]

    def gather_y(k):
        arrived(block(k, 0, SHARE[k], 15, tile), 7, k)
        for h in range(2):
            mine = piece(k, 0, h)
            remote(mine, mine, 8, k, up)
            remote(mine, mine, 11, k, down)
            remote(mine, mine, 9, k, partner)

    def forward(k):
        arrived(block(k, 0, SHARE[k], 8, 2 * tile), 8, k)
        below = [piece(k, 3, h) for h in range(2)]
        remote(below[0], below[0], 12, k, up)
        arrived(block(k, 0, SHARE[k], 8, 2 * tile), 11, k)
        above = [piece(k, 1, h) for h in range(2)]
        remote(above[1], above[1], 12, k, down)
        for ref in below + above:
            remote(ref, ref, 9, k, partner)

    def gather_core(k):
        arrived(block(k, 0, SHARE[k], 8, 2 * tile), 12, k)
        for h in range(2):
            far = piece(k, 2, h)
            remote(far, far, 9, k, partner)

    def spread(k):
        arrived(block(k, SHARE[k], 4, 3, tile), 13, k)
        for h in range(2):
            mine = out.at[SHARE[k]:4, c, zh, x, :, columns(k, zl, h)]
            for n in (2, 1, 3):
                zz = lax.rem(z + n, 4)
                device = (zz // 2, x, c, lax.rem(zz, 2), y) if h else (zh, lax.rem(x + n, 4), c, zl, y)
                remote(mine, mine, 16 if h else 14, k, device)

    def columns(k, zzl, h):
        return pl.ds(pl.multiple_of(k * width + zzl * half + h * (half // 2), 128), half // 2)

    def cross(k):
        arrived(block(k, SHARE[k], 4, 3, half // 2), 14, k)
        row = out.at[SHARE[k]:4, c, zh, :, :, columns(k, zl, 0)]
        for n in (2, 1, 3):
            zz = lax.rem(z + n, 4)
            remote(row, row, 17, k, (zz // 2, x, c, lax.rem(zz, 2), y))
        arrived(block(k, SHARE[k], 4, 3, half // 2), 16, k)
        for n in (2, 1, 3):
            for h in range(2):
                line = out.at[SHARE[k]:4, c, :, x, :, columns(k, h, 1)]
                remote(line, line, 17, k, (zh, lax.rem(x + n, 4), c, zl, y))

    def spread_core(k):
        arrived(block(k, SHARE[k], 4, 12, half), 17, k)
        mine = out.at[SHARE[k]:4, c, :, :, :, cols(k)]
        remote(mine, mine, 15, k, partner)

    def sent(count, stage):
        for ref, most in ((pre, (CHUNKS, 16, 8)), (col, (CHUNKS, 3, 2, 2, 4, 8))):
            for dims in itertools.product(*[range(1, m + 1) for m in most]):
                if math.prod(dims) == count:
                    ref = ref.at[tuple(slice(0, d) for d in dims[:-1]) + (slice(None), slice(0, dims[-1] * tile))]
                    pltpu.make_async_copy(ref, ref, send.at[stage]).wait()
                    return
        assert count == 0

    def finish():
        for k in range(CHUNKS):
            s = SHARE[k]
            if s > 0:
                arrived(block(k, 0, s, 8, width), 9, k)
            if s < 4:
                arrived(block(k, s, 4, 8, width), 15, k)
        s = sum(SHARE)
        rest = 4 * CHUNKS - s
        once = {0: 15 * 8, 1: 7, 2: 7, 3: 15 * 8, 4: 3 * 8 * 8, 5: 2 * 3 * 4 * 2, 10: 2 * 3 * 8 * 2, 6: 15 * 3}
        for stage, count in once.items():
            sent(CHUNKS * count, stage)
        for stage, count in {7: 15, 8: 16, 11: 16, 12: 16}.items():
            sent(s * count, stage)
        sent(s * 64, 9)
        for stage, count in {13: 3, 14: 6, 16: 6, 17: 48, 15: 64}.items():
            sent(rest * count, stage)

    def load():
        for k in range(CHUNKS):
            own_color(k).start()
        for cp in ranks:
            cp.wait()
        tab.extend(tables())

    tab = []
    stages = dict(alpha=alpha, prefix=prefix, group=group, trans=trans, scale=scale, sum_core=sum_core, around=around, sum_y=sum_y,
                  sum_xz=sum_xz, gather_y=gather_y, forward=forward, gather_core=gather_core, spread=spread, cross=cross,
                  spread_core=spread_core)
    ranks = [pltpu.make_async_copy(depth_in, depth, own.at[2, 0]), pltpu.make_async_copy(bricks_in, bricks, own.at[2, 1])]
    for cp in ranks:
        cp.start()
    meet()
    for name in PLAN:
        with jax.named_scope(name):
            if name == "load":
                load()
            elif name == "finish":
                finish()
            elif name[-1] == "a":
                alpha(int(name[-2]), 0, 7)
            elif name[-1] == "b":
                alpha(int(name[-2]), 7, 15)
            else:
                stages[name[:-1]](int(name[-1]))


def local(images, depth, brick_map):
    channels, rows, columns = images.shape[1:]
    width = columns // CHUNKS
    tile, half = width // 8, width // 2
    f = jnp.float32
    n = CHUNKS
    vm = lambda *s: pltpu.VMEM(s, f)
    out = pl.pallas_call(
        kernel,
        out_shape=pltpu.VMEM((channels, 2, 2, 4, ROW, columns), f),
        in_specs=[pl.BlockSpec(memory_space=pl.ANY)] * 3,
        out_specs=pl.BlockSpec(memory_space=pltpu.VMEM),
        scratch_shapes=[
            *[vm(16, ROW, width)] * n, *[vm(8, ROW, tile)] * n,
            vm(n, 16, ROW, width), vm(n, 8, ROW, tile), vm(n, 8, ROW, tile), vm(n, 8, ROW, tile), vm(n, 8, ROW, tile),
            vm(n, 16, ROW, width), vm(n, 16, ROW, width),
            vm(n, 3, 2, 2, 4, ROW, width), vm(n, 3, 8, ROW, width), vm(n, 3, 8, ROW, width), vm(n, 3, 8, 2, ROW, half),
            vm(n, 2, 3, 4, 2, ROW, tile), vm(n, 2, 3, 4, 2, ROW, tile), vm(n, 2, 3, 8, 2, ROW, tile), vm(n, 3, 8, 2, ROW, tile), vm(n, 15, 3, ROW, tile),
            pltpu.SemaphoreType.DMA((18,)), pltpu.SemaphoreType.DMA((18, n)), pltpu.SemaphoreType.DMA((3, n)),
            pltpu.SMEM(depth.shape, jnp.int32), pltpu.SMEM(brick_map.shape, jnp.int32),
        ],
        compiler_params=pltpu.CompilerParams(has_side_effects=True, collective_id=0, vmem_limit_bytes=48 * 2**20),
    )(depth, brick_map, images.reshape(channels, 2, 2, 4, ROW, columns))
    return out.reshape(channels, rows, columns)


def solution(mesh):
    torus = Mesh(mesh.devices.reshape(2, 4, 2, 2, 4), AXES)
    return jax.shard_map(
        local,
        mesh=torus,
        in_specs=(P(("zh", "x", "c", "zl", "y"), None, None, None), P(), P()),
        out_specs=P(),
        check_vma=False,
    )
```

```python
import functools
import itertools
import math

import jax
import jax.numpy as jnp
from jax import lax
from jax.experimental import pallas as pl
from jax.experimental.pallas import tpu as pltpu
from jax.sharding import Mesh
from jax.sharding import PartitionSpec as P

AXES = ("zh", "x", "c", "zl", "y")
CHUNKS = 4
SHARE = (4, 2, 2, 2)
ROW = 8
MESH = pl.DeviceIdType.MESH

AA_ORDER = [(0, 0, 1), (0, 1, 0), (0, 1, 1), (1, 0, 0), (3, 1, 0), (2, 0, 0), (1, 1, 0), (3, 0, 0), (2, 1, 0),
            (1, 0, 1), (3, 1, 1), (2, 0, 1), (1, 1, 1), (3, 0, 1), (2, 1, 1)]
BA_ORDER = [(dy, dz) for dy in (2, 1, 3, 0) for dz in (1, 0) if (dy, dz) != (0, 0)]
XZ_ORDER = [(dx, dz) for dx, dz in
            ((2, 2), (1, 2), (3, 2), (2, 1), (2, 3), (1, 1), (3, 3), (1, 3), (3, 1),
             (0, 2), (2, 0), (1, 0), (0, 1), (3, 0), (0, 3))]

PLAN = (
    "alpha0", "load", "alpha1", "prefix0", "alpha2", "group0", "prefix1", "alpha3", "group1", "prefix2",
    "trans0", "prefix3", "group2", "trans1", "scale0", "group3", "sum_core0", "trans2", "scale1", "around0",
    "sum_core1", "trans3", "scale2", "around1", "sum_core2", "sum_y0", "scale3", "sum_y1", "around2",
    "sum_xz0", "sum_core3", "sum_xz1", "around3", "sum_y2", "gather_y0", "spread1", "sum_y3", "sum_xz2",
    "gather_y1", "cross1", "spread2", "sum_xz3", "forward0", "gather_y2", "spread3", "spread_core1", "cross2",
    "gather_y3", "gather_core0", "forward1", "cross3", "forward2", "spread_core2", "forward3", "gather_core1",
    "spread_core3", "gather_core2", "gather_core3", "finish",
)


def kernel(depth_in, bricks_in, img, out, *scratch):
    ain, gin = scratch[:CHUNKS], scratch[CHUNKS:2 * CHUNKS]
    pre, gb, qb, qout, qin, tout, tin, col, cs, cin, a1, ys, b1, yin, a2, xin, send, recv, own, depth, bricks = scratch[2 * CHUNKS:]
    zh, x, c, zl, y = (lax.axis_index(a) for a in AXES)
    z = zh * 2 + zl
    width = tin.shape[-1]
    tile = width // 8
    half = width // 2
    band = c * 8 + zh * 4 + x
    slot_b = zl * 4 + y

    def remote(src, dst, stage, k, device):
        cp = pltpu.make_async_remote_copy(
            src_ref=src, dst_ref=dst, send_sem=send.at[stage], recv_sem=recv.at[stage, k],
            device_id=device, device_id_type=MESH)
        cp.start()

    def arrived(ref, stage, k):
        pltpu.make_async_copy(ref, ref, recv.at[stage, k]).wait()

    def aa_peers():
        for dx, dz, dc in AA_ORDER:
            xx, zz, cc = lax.rem(x + dx, 4), lax.rem(zh + dz, 2), lax.rem(c + dc, 2)
            yield cc * 8 + zz * 4 + xx, (zz, xx, cc, zl, y)

    def ba_peers():
        for dy, dz in BA_ORDER:
            yy, zz = lax.rem(y + dy, 4), lax.rem(zl + dz, 2)
            yield zz * 4 + yy, (zh, x, c, zz, yy)

    def xz_peers():
        for n, (dx, dz) in enumerate(XZ_ORDER):
            xx, zz = lax.rem(x + dx, 4), lax.rem(z + dz, 4)
            yield n, zz // 2 * 4 + xx, lax.rem(zz, 2), (zz // 2, xx, c, lax.rem(zz, 2), y)

    partner = (zh, x, 1 - c, zl, y)

    up = (zh, x, c, zl, lax.rem(y + 1, 4))
    down = (zh, x, c, zl, lax.rem(y + 3, 4))

    def meet():
        barrier = pltpu.get_barrier_semaphore()
        devices = [d for _, d in aa_peers()] + [d for _, d in ba_peers()]
        devices += [(zz // 2, xx, c, lax.rem(zz, 2), y) for xx, zz in
                    ((lax.rem(x + dx, 4), lax.rem(z + dz, 4)) for dx in range(4) for dz in (1, 3))]
        for device in devices:
            pl.semaphore_signal(barrier, inc=1, device_id=device, device_id_type=MESH)
        pl.semaphore_wait(barrier, len(devices))

    def tables():
        def rank_of(zz, xx, cc, zzl, yy):
            return depth[bricks[(((zz * 4 + xx) * 2 + cc) * 2 + zzl) * 4 + yy]]

        inner = [lax.rem(rank_of(r // 4 % 2, r % 4, r // 8, zl, y), 16) for r in range(16)]
        group = [lax.div(rank_of(zh, x, c, j // 4, j % 4), 16) for j in range(8)]

        def inverse(ranks, m):
            return functools.reduce(lambda a, iv: jnp.where(iv[1] == m, iv[0], a), enumerate(ranks), 0)

        return ([inverse(inner, m) for m in range(16)] + inner
                + [inverse(group, m) for m in range(8)] + group)

    def cols(k):
        return pl.ds(k * width, width)

    def own_alpha(k):
        return pltpu.make_async_copy(img.at[3, c, zh, x, :, cols(k)], ain[k].at[band], own.at[0, k])

    def own_color(k):
        return pltpu.make_async_copy(img.at[0:3, :, :, :, :, cols(k)], col.at[k], own.at[1, k])

    def alpha(k, begin=0, end=15):
        for (zz, xx, cc, _, _), device in [(d, d) for _, d in aa_peers()][begin:end]:
            remote(img.at[3, cc, zz, xx, :, cols(k)], ain[k].at[band], 0, k, device)
        if begin == 0:
            own_alpha(k).start()

    def prefix(k):
        own_alpha(k).wait()
        arrived(ain[k].at[pl.ds(0, 15)], 0, k)
        run = jnp.ones((ROW, width), jnp.float32)
        for m in range(16):
            pre[k, m] = run
            run = run * (1.0 - ain[k][tab[m]])
        for j in range(8):
            gb[k, j] = run[:, j * tile:(j + 1) * tile]
        gin[k][slot_b] = gb[k, slot_b]
        for j, device in ba_peers():
            remote(gb.at[k, j], gin[k].at[slot_b], 1, k, device)

    def group(k):
        arrived(gin[k].at[pl.ds(0, 7)], 1, k)
        run = jnp.ones((ROW, tile), jnp.float32)
        for m in range(8):
            qb[k, m] = run
            run = run * gin[k][tab[32 + m]]
        out[3, c, zh, x, :, strip(k)] = 1.0 - run
        for j in range(8):
            qout[k, j] = qb[k, tab[40 + j]]
        qin[k, slot_b] = qout[k, slot_b]
        for j, device in ba_peers():
            remote(qout.at[k, j], qin.at[k, slot_b], 2, k, device)

    def trans(k):
        arrived(qin.at[k, pl.ds(0, 7)], 2, k)
        q = jnp.concatenate([qin[k, j] for j in range(8)], axis=1)
        for r in range(16):
            tout[k, r] = pre[k, tab[16 + r]] * q
        tin[k, band] = tout[k, band]
        for r, device in aa_peers():
            remote(tout.at[k, r], tin.at[k, band], 3, k, device)

    def scale(k):
        own_color(k).wait()
        arrived(tin.at[k, pl.ds(0, 15)], 3, k)

        def body(i, carry):
            r = (1 - c) * 8 + i
            t = tin[k, r]
            for ch in range(3):
                cs[k, ch, i] = col[k, ch, 1 - c, i // 4, i % 4] * t
            return carry

        lax.fori_loop(0, 8, body, 0)
        remote(cs.at[k], cin.at[k], 4, k, partner)

    def sum_core(k):
        arrived(cin.at[k], 4, k)

        def body(i, carry):
            r = c * 8 + i
            t = tin[k, r]
            for ch in range(3):
                v = col[k, ch, c, i // 4, i % 4] * t + cin[k, ch, i]
                a1[k, ch, i, 0] = v[:, :half]
                a1[k, ch, i, 1] = v[:, half:]
            return carry

        lax.fori_loop(0, 8, body, 0)
        def part(dy, h):
            return a1.at[k, :, 4 * h:4 * h + 4, :, :, tiles(dy)]

        remote(part(2, 0), ys.at[k, 0], 5, k, up)
        remote(part(2, 1), ys.at[k, 1], 5, k, down)
        remote(part(1, 1), yin.at[k, 0, :, 4:8], 10, k, up)
        remote(part(3, 0), yin.at[k, 1, :, 0:4], 10, k, down)

    def tiles(dy):
        return pl.ds(pl.multiple_of(lax.rem(y + dy, 4) * tile, 128), tile)

    def around(k):
        arrived(ys.at[k], 5, k)
        for n, dy, device in ((0, 1, up), (1, 3, down)):
            for ch in range(3):
                for i in range(4):
                    b1[k, n, ch, i] = a1[k, ch, 4 * n + i, :, :, tiles(dy)] + ys[k, n, ch, i]
            remote(b1.at[k, n], yin.at[k, n, :, 4 * n:4 * n + 4], 10, k, device)

    def sum_y(k):
        arrived(yin.at[k], 10, k)

        def body(i, carry):
            for ch in range(3):
                a2[k, ch, i] = a1[k, ch, i, :, :, tiles(0)] + (yin[k, 0, ch, i] + yin[k, 1, ch, i])
            return carry

        lax.fori_loop(0, 8, body, 0)
        for n, r, t, device in xz_peers():
            remote(a2.at[k, :, r, t], xin.at[k, n], 6, k, device)

    def strip(k):
        return pl.ds(pl.multiple_of(k * width + slot_b * tile, 128), tile)

    def sum_xz(k):
        arrived(xin.at[k], 6, k)
        for ch in range(3):
            v = a2[k, ch, zh * 4 + x, zl]
            for n in range(15):
                v = v + xin[k, n, ch]
            out[ch, c, zh, x, :, strip(k)] = v
        if SHARE[k] < 4:
            mine = out.at[SHARE[k]:4, c, zh, x, :, strip(k)]
            for dy in (2, 1, 3):
                remote(mine, mine, 13, k, (zh, x, c, zl, lax.rem(y + dy, 4)))
        if SHARE[k] > 0:
            mine = out.at[0:SHARE[k], c, zh, x, :, strip(k)]
            for n, r, t, device in xz_peers():
                remote(mine, mine, 7, k, device)

    def block(k, first, last, count, columns):
        return pre.at[0:last - first, 0:count, :, 0:columns]

    def piece(k, dy, h):
        at = pl.multiple_of(k * width + h * half + lax.rem(y + dy, 4) * tile, 128)
        return out.at[0:SHARE[k], c, :, :, :, pl.ds(at, tile)]

    def gather_y(k):
        arrived(block(k, 0, SHARE[k], 15, tile), 7, k)
        for h in range(2):
            mine = piece(k, 0, h)
            remote(mine, mine, 8, k, up)
            remote(mine, mine, 11, k, down)
            remote(mine, mine, 9, k, partner)

    def forward(k):
        arrived(block(k, 0, SHARE[k], 8, 2 * tile), 8, k)
        below = [piece(k, 3, h) for h in range(2)]
        remote(below[0], below[0], 12, k, up)
        arrived(block(k, 0, SHARE[k], 8, 2 * tile), 11, k)
        above = [piece(k, 1, h) for h in range(2)]
        remote(above[1], above[1], 12, k, down)
        for ref in below + above:
            remote(ref, ref, 9, k, partner)

    def gather_core(k):
        arrived(block(k, 0, SHARE[k], 8, 2 * tile), 12, k)
        for h in range(2):
            far = piece(k, 2, h)
            remote(far, far, 9, k, partner)

    def spread(k):
        arrived(block(k, SHARE[k], 4, 3, tile), 13, k)
        for h in range(2):
            mine = out.at[SHARE[k]:4, c, zh, x, :, columns(k, zl, h)]
            for n in (2, 1, 3):
                zz = lax.rem(z + n, 4)
                device = (zz // 2, x, c, lax.rem(zz, 2), y) if h else (zh, lax.rem(x + n, 4), c, zl, y)
                remote(mine, mine, 16 if h else 14, k, device)

    def columns(k, zzl, h):
        return pl.ds(pl.multiple_of(k * width + zzl * half + h * (half // 2), 128), half // 2)

    def cross(k):
        arrived(block(k, SHARE[k], 4, 3, half // 2), 14, k)
        row = out.at[SHARE[k]:4, c, zh, :, :, columns(k, zl, 0)]
        for n in (2, 1, 3):
            zz = lax.rem(z + n, 4)
            remote(row, row, 17, k, (zz // 2, x, c, lax.rem(zz, 2), y))
        arrived(block(k, SHARE[k], 4, 3, half // 2), 16, k)
        for n in (2, 1, 3):
            for h in range(2):
                line = out.at[SHARE[k]:4, c, :, x, :, columns(k, h, 1)]
                remote(line, line, 17, k, (zh, lax.rem(x + n, 4), c, zl, y))

    def spread_core(k):
        arrived(block(k, SHARE[k], 4, 12, half), 17, k)
        mine = out.at[SHARE[k]:4, c, :, :, :, cols(k)]
        remote(mine, mine, 15, k, partner)

    def sent(count, stage):
        for ref, most in ((pre, (CHUNKS, 16, 8)), (col, (CHUNKS, 3, 2, 2, 4, 8))):
            for dims in itertools.product(*[range(1, m + 1) for m in most]):
                if math.prod(dims) == count:
                    ref = ref.at[tuple(slice(0, d) for d in dims[:-1]) + (slice(None), slice(0, dims[-1] * tile))]
                    pltpu.make_async_copy(ref, ref, send.at[stage]).wait()
                    return
        assert count == 0

    def finish():
        for k in range(CHUNKS):
            s = SHARE[k]
            if s > 0:
                arrived(block(k, 0, s, 8, width), 9, k)
            if s < 4:
                arrived(block(k, s, 4, 8, width), 15, k)
        s = sum(SHARE)
        rest = 4 * CHUNKS - s
        once = {0: 15 * 8, 1: 7, 2: 7, 3: 15 * 8, 4: 3 * 8 * 8, 5: 2 * 3 * 4 * 2, 10: 2 * 3 * 8 * 2, 6: 15 * 3}
        for stage, count in once.items():
            sent(CHUNKS * count, stage)
        for stage, count in {7: 15, 8: 16, 11: 16, 12: 16}.items():
            sent(s * count, stage)
        sent(s * 64, 9)
        for stage, count in {13: 3, 14: 6, 16: 6, 17: 48, 15: 64}.items():
            sent(rest * count, stage)

    def load():
        for k in range(CHUNKS):
            own_color(k).start()
        for cp in ranks:
            cp.wait()
        tab.extend(tables())

    tab = []
    stages = dict(alpha=alpha, prefix=prefix, group=group, trans=trans, scale=scale, sum_core=sum_core, around=around, sum_y=sum_y,
                  sum_xz=sum_xz, gather_y=gather_y, forward=forward, gather_core=gather_core, spread=spread, cross=cross,
                  spread_core=spread_core)
    ranks = [pltpu.make_async_copy(depth_in, depth, own.at[2, 0]), pltpu.make_async_copy(bricks_in, bricks, own.at[2, 1])]
    for cp in ranks:
        cp.start()
    meet()
    for name in PLAN:
        with jax.named_scope(name):
            if name == "load":
                load()
            elif name == "finish":
                finish()
            elif name[-1] == "a":
                alpha(int(name[-2]), 0, 7)
            elif name[-1] == "b":
                alpha(int(name[-2]), 7, 15)
            else:
                stages[name[:-1]](int(name[-1]))


def local(images, depth, brick_map):
    channels, rows, columns = images.shape[1:]
    width = columns // CHUNKS
    tile, half = width // 8, width // 2
    f = jnp.float32
    n = CHUNKS
    vm = lambda *s: pltpu.VMEM(s, f)
    out = pl.pallas_call(
        kernel,
        out_shape=pltpu.VMEM((channels, 2, 2, 4, ROW, columns), f),
        in_specs=[pl.BlockSpec(memory_space=pl.ANY)] * 3,
        out_specs=pl.BlockSpec(memory_space=pltpu.VMEM),
        scratch_shapes=[
            *[vm(16, ROW, width)] * n, *[vm(8, ROW, tile)] * n,
            vm(n, 16, ROW, width), vm(n, 8, ROW, tile), vm(n, 8, ROW, tile), vm(n, 8, ROW, tile), vm(n, 8, ROW, tile),
            vm(n, 16, ROW, width), vm(n, 16, ROW, width),
            vm(n, 3, 2, 2, 4, ROW, width), vm(n, 3, 8, ROW, width), vm(n, 3, 8, ROW, width), vm(n, 3, 8, 2, ROW, half),
            vm(n, 2, 3, 4, 2, ROW, tile), vm(n, 2, 3, 4, 2, ROW, tile), vm(n, 2, 3, 8, 2, ROW, tile), vm(n, 3, 8, 2, ROW, tile), vm(n, 15, 3, ROW, tile),
            pltpu.SemaphoreType.DMA((18,)), pltpu.SemaphoreType.DMA((18, n)), pltpu.SemaphoreType.DMA((3, n)),
            pltpu.SMEM(depth.shape, jnp.int32), pltpu.SMEM(brick_map.shape, jnp.int32),
        ],
        compiler_params=pltpu.CompilerParams(has_side_effects=True, collective_id=0, vmem_limit_bytes=48 * 2**20),
    )(depth, brick_map, images.reshape(channels, 2, 2, 4, ROW, columns))
    return out.reshape(channels, rows, columns)


def solution(mesh):
    torus = Mesh(mesh.devices.reshape(2, 4, 2, 2, 4), AXES)
    return jax.shard_map(
        local,
        mesh=torus,
        in_specs=(P(("zh", "x", "c", "zl", "y"), None, None, None), P(), P()),
        out_specs=P(),
        check_vma=False,
    )
```

```python
import functools
import itertools
import math

import jax
import jax.numpy as jnp
from jax import lax
from jax.experimental import pallas as pl
from jax.experimental.pallas import tpu as pltpu
from jax.sharding import Mesh
from jax.sharding import PartitionSpec as P

AXES = ("zh", "x", "c", "zl", "y")
CHUNKS = 4
SHARE = (4, 2, 2, 2)
ROW = 8
MESH = pl.DeviceIdType.MESH

AA_ORDER = [(0, 0, 1), (0, 1, 0), (0, 1, 1), (1, 0, 0), (3, 1, 0), (2, 0, 0), (1, 1, 0), (3, 0, 0), (2, 1, 0),
            (1, 0, 1), (3, 1, 1), (2, 0, 1), (1, 1, 1), (3, 0, 1), (2, 1, 1)]
BA_ORDER = [(dy, dz) for dy in (2, 1, 3, 0) for dz in (1, 0) if (dy, dz) != (0, 0)]
XZ_ORDER = [(dx, dz) for dx, dz in
            ((2, 2), (1, 2), (3, 2), (2, 1), (2, 3), (1, 1), (3, 3), (1, 3), (3, 1),
             (0, 2), (2, 0), (1, 0), (0, 1), (3, 0), (0, 3))]

PLAN = (
    "alpha0", "load", "alpha1", "prefix0", "alpha2", "group0", "prefix1", "alpha3", "group1", "prefix2",
    "trans0", "prefix3", "group2", "trans1", "scale0", "group3", "sum_core0", "trans2", "scale1", "around0",
    "sum_core1", "trans3", "scale2", "around1", "sum_core2", "sum_y0", "scale3", "sum_y1", "around2",
    "sum_xz0", "sum_core3", "sum_xz1", "around3", "sum_y2", "gather_y0", "spread1", "sum_y3", "sum_xz2",
    "gather_y1", "cross1", "spread2", "sum_xz3", "forward0", "gather_y2", "spread3", "spread_core1", "cross2",
    "gather_y3", "gather_core0", "forward1", "cross3", "forward2", "spread_core2", "forward3", "gather_core1",
    "spread_core3", "gather_core2", "gather_core3", "finish",
)


def kernel(depth_in, bricks_in, img, out, *scratch):
    ain, gin = scratch[:CHUNKS], scratch[CHUNKS:2 * CHUNKS]
    pre, gb, qb, qout, qin, tout, tin, col, cs, cin, a1, ys, b1, yin, a2, xin, send, recv, own, depth, bricks = scratch[2 * CHUNKS:]
    zh, x, c, zl, y = (lax.axis_index(a) for a in AXES)
    z = zh * 2 + zl
    width = tin.shape[-1]
    tile = width // 8
    half = width // 2
    band = c * 8 + zh * 4 + x
    slot_b = zl * 4 + y

    def remote(src, dst, stage, k, device):
        cp = pltpu.make_async_remote_copy(
            src_ref=src, dst_ref=dst, send_sem=send.at[stage], recv_sem=recv.at[stage, 0 if stage in (9, 15) else k],
            device_id=device, device_id_type=MESH)
        cp.start()

    def arrived(ref, stage, k):
        pltpu.make_async_copy(ref, ref, recv.at[stage, k]).wait()

    def aa_peers():
        for dx, dz, dc in AA_ORDER:
            xx, zz, cc = lax.rem(x + dx, 4), lax.rem(zh + dz, 2), lax.rem(c + dc, 2)
            yield cc * 8 + zz * 4 + xx, (zz, xx, cc, zl, y)

    def ba_peers():
        for dy, dz in BA_ORDER:
            yy, zz = lax.rem(y + dy, 4), lax.rem(zl + dz, 2)
            yield zz * 4 + yy, (zh, x, c, zz, yy)

    def xz_peers():
        for n, (dx, dz) in enumerate(XZ_ORDER):
            xx, zz = lax.rem(x + dx, 4), lax.rem(z + dz, 4)
            yield n, zz // 2 * 4 + xx, lax.rem(zz, 2), (zz // 2, xx, c, lax.rem(zz, 2), y)

    partner = (zh, x, 1 - c, zl, y)

    up = (zh, x, c, zl, lax.rem(y + 1, 4))
    down = (zh, x, c, zl, lax.rem(y + 3, 4))

    def meet():
        barrier = pltpu.get_barrier_semaphore()
        devices = [(zz // 2, xx, c, lax.rem(zz, 2), y) for xx, zz in
                    ((lax.rem(x + dx, 4), lax.rem(z + dz, 4)) for dx in (2, 1, 3, 0) for dz in (3, 1))]
        devices = [d for _, d in aa_peers()][::-1] + devices + [d for _, d in ba_peers()]
        for device in devices:
            pl.semaphore_signal(barrier, inc=1, device_id=device, device_id_type=MESH)
        pl.semaphore_wait(barrier, len(devices))

    def tables():
        def rank_of(zz, xx, cc, zzl, yy):
            return depth[bricks[(((zz * 4 + xx) * 2 + cc) * 2 + zzl) * 4 + yy]]

        inner = [lax.rem(rank_of(r // 4 % 2, r % 4, r // 8, zl, y), 16) for r in range(16)]
        group = [lax.div(rank_of(zh, x, c, j // 4, j % 4), 16) for j in range(8)]

        def inverse(ranks, m):
            return functools.reduce(lambda a, iv: jnp.where(iv[1] == m, iv[0], a), enumerate(ranks), 0)

        return ([inverse(inner, m) for m in range(16)] + inner
                + [inverse(group, m) for m in range(8)] + group)

    def cols(k):
        return pl.ds(k * width, width)

    def own_alpha(k):
        return pltpu.make_async_copy(img.at[3, c, zh, x, :, cols(k)], ain[k].at[band], own.at[0, k])

    def own_color(k):
        return pltpu.make_async_copy(img.at[0:3, :, :, :, :, cols(k)], col.at[k], own.at[1, k])

    def alpha(k, begin=0, end=15):
        for (zz, xx, cc, _, _), device in [(d, d) for _, d in aa_peers()][begin:end]:
            remote(img.at[3, cc, zz, xx, :, cols(k)], ain[k].at[band], 0, k, device)
        if begin == 0:
            own_alpha(k).start()

    def prefix(k):
        own_alpha(k).wait()
        arrived(ain[k].at[pl.ds(0, 15)], 0, k)
        run = jnp.ones((ROW, width), jnp.float32)
        for m in range(16):
            pre[k, m] = run
            run = run * (1.0 - ain[k][tab[m]])
        for j in range(8):
            gb[k, j] = run[:, j * tile:(j + 1) * tile]
        gin[k][slot_b] = gb[k, slot_b]
        for j, device in ba_peers():
            remote(gb.at[k, j], gin[k].at[slot_b], 1, k, device)

    def group(k):
        arrived(gin[k].at[pl.ds(0, 7)], 1, k)
        run = jnp.ones((ROW, tile), jnp.float32)
        for m in range(8):
            qb[k, m] = run
            run = run * gin[k][tab[32 + m]]
        out[3, c, zh, x, :, strip(k)] = 1.0 - run
        for j in range(8):
            qout[k, j] = qb[k, tab[40 + j]]
        qin[k, slot_b] = qout[k, slot_b]
        for j, device in ba_peers():
            remote(qout.at[k, j], qin.at[k, slot_b], 2, k, device)

    def trans(k):
        arrived(qin.at[k, pl.ds(0, 7)], 2, k)
        q = jnp.concatenate([qin[k, j] for j in range(8)], axis=1)
        for r in range(16):
            tout[k, r] = pre[k, tab[16 + r]] * q
        tin[k, band] = tout[k, band]
        for r, device in aa_peers():
            remote(tout.at[k, r], tin.at[k, band], 3, k, device)

    def scale(k):
        own_color(k).wait()
        arrived(tin.at[k, pl.ds(0, 15)], 3, k)

        def body(i, carry):
            r = (1 - c) * 8 + i
            t = tin[k, r]
            for ch in range(3):
                cs[k, ch, i] = col[k, ch, 1 - c, i // 4, i % 4] * t
            return carry

        lax.fori_loop(0, 8, body, 0)
        remote(cs.at[k], cin.at[k], 4, k, partner)

    def sum_core(k):
        arrived(cin.at[k], 4, k)

        def body(i, carry):
            r = c * 8 + i
            t = tin[k, r]
            for ch in range(3):
                v = col[k, ch, c, i // 4, i % 4] * t + cin[k, ch, i]
                a1[k, ch, i, 0] = v[:, :half]
                a1[k, ch, i, 1] = v[:, half:]
            return carry

        lax.fori_loop(0, 8, body, 0)
        def part(dy, h):
            return a1.at[k, :, 4 * h:4 * h + 4, :, :, tiles(dy)]

        remote(part(2, 0), ys.at[k, 0], 5, k, up)
        remote(part(2, 1), ys.at[k, 1], 5, k, down)
        remote(part(1, 1), yin.at[k, 0, :, 4:8], 10, k, up)
        remote(part(3, 0), yin.at[k, 1, :, 0:4], 10, k, down)

    def tiles(dy):
        return pl.ds(pl.multiple_of(lax.rem(y + dy, 4) * tile, 128), tile)

    def around(k):
        arrived(ys.at[k], 5, k)
        for n, dy, device in ((0, 1, up), (1, 3, down)):
            for ch in range(3):
                for i in range(4):
                    b1[k, n, ch, i] = a1[k, ch, 4 * n + i, :, :, tiles(dy)] + ys[k, n, ch, i]
            remote(b1.at[k, n], yin.at[k, n, :, 4 * n:4 * n + 4], 10, k, device)

    def sum_y(k):
        arrived(yin.at[k], 10, k)

        def body(i, carry):
            for ch in range(3):
                a2[k, ch, i] = a1[k, ch, i, :, :, tiles(0)] + (yin[k, 0, ch, i] + yin[k, 1, ch, i])
            return carry

        lax.fori_loop(0, 8, body, 0)
        for n, r, t, device in xz_peers():
            remote(a2.at[k, :, r, t], xin.at[k, n], 6, k, device)

    def strip(k):
        return pl.ds(pl.multiple_of(k * width + slot_b * tile, 128), tile)

    def sum_xz(k):
        arrived(xin.at[k], 6, k)
        for ch in range(3):
            v = a2[k, ch, zh * 4 + x, zl]
            for n in range(15):
                v = v + xin[k, n, ch]
            out[ch, c, zh, x, :, strip(k)] = v
        if SHARE[k] < 4:
            mine = out.at[SHARE[k]:4, c, zh, x, :, strip(k)]
            for dy in (2, 1, 3):
                remote(mine, mine, 13, k, (zh, x, c, zl, lax.rem(y + dy, 4)))
        if SHARE[k] > 0:
            mine = out.at[0:SHARE[k], c, zh, x, :, strip(k)]
            for n, r, t, device in xz_peers():
                remote(mine, mine, 7, k, device)

    def block(k, first, last, count, columns):
        return pre.at[0:last - first, 0:count, :, 0:columns]

    def piece(k, dy, h):
        at = pl.multiple_of(k * width + h * half + lax.rem(y + dy, 4) * tile, 128)
        return out.at[0:SHARE[k], c, :, :, :, pl.ds(at, tile)]

    def gather_y(k):
        arrived(block(k, 0, SHARE[k], 15, tile), 7, k)
        for h in range(2):
            mine = piece(k, 0, h)
            remote(mine, mine, 8, k, up)
            remote(mine, mine, 11, k, down)
            remote(mine, mine, 9, k, partner)

    def forward(k):
        arrived(block(k, 0, SHARE[k], 8, 2 * tile), 8, k)
        below = [piece(k, 3, h) for h in range(2)]
        remote(below[0], below[0], 12, k, up)
        arrived(block(k, 0, SHARE[k], 8, 2 * tile), 11, k)
        above = [piece(k, 1, h) for h in range(2)]
        remote(above[1], above[1], 12, k, down)
        for ref in below + above:
            remote(ref, ref, 9, k, partner)

    def gather_core(k):
        arrived(block(k, 0, SHARE[k], 8, 2 * tile), 12, k)
        for h in range(2):
            far = piece(k, 2, h)
            remote(far, far, 9, k, partner)

    def spread(k):
        arrived(block(k, SHARE[k], 4, 3, tile), 13, k)
        for h in range(2):
            mine = out.at[SHARE[k]:4, c, zh, x, :, columns(k, zl, h)]
            for n in (2, 1, 3):
                zz = lax.rem(z + n, 4)
                device = (zz // 2, x, c, lax.rem(zz, 2), y) if h else (zh, lax.rem(x + n, 4), c, zl, y)
                remote(mine, mine, 16 if h else 14, k, device)

    def columns(k, zzl, h):
        return pl.ds(pl.multiple_of(k * width + zzl * half + h * (half // 2), 128), half // 2)

    def cross(k):
        arrived(block(k, SHARE[k], 4, 3, half // 2), 14, k)
        row = out.at[SHARE[k]:4, c, zh, :, :, columns(k, zl, 0)]
        for n in (2, 1, 3):
            zz = lax.rem(z + n, 4)
            remote(row, row, 17, k, (zz // 2, x, c, lax.rem(zz, 2), y))
        arrived(block(k, SHARE[k], 4, 3, half // 2), 16, k)
        for n in (2, 1, 3):
            for h in range(2):
                line = out.at[SHARE[k]:4, c, :, x, :, columns(k, h, 1)]
                remote(line, line, 17, k, (zh, lax.rem(x + n, 4), c, zl, y))

    def spread_core(k):
        arrived(block(k, SHARE[k], 4, 12, half), 17, k)
        mine = out.at[SHARE[k]:4, c, :, :, :, cols(k)]
        remote(mine, mine, 15, k, partner)

    def sent(count, stage, sem=None):
        for ref, most in ((pre, (CHUNKS, 16, 8)), (col, (CHUNKS, 3, 2, 2, 4, 8))):
            for dims in itertools.product(*[range(1, m + 1) for m in most]):
                if math.prod(dims) == count:
                    ref = ref.at[tuple(slice(0, d) for d in dims[:-1]) + (slice(None), slice(0, dims[-1] * tile))]
                    pltpu.make_async_copy(ref, ref, send.at[stage] if sem is None else sem).wait()
                    return
        assert count == 0

    def finish():
        s = sum(SHARE)
        rest = 4 * CHUNKS - s
        sent(s * 64, 9, recv.at[9, 0])
        sent(rest * 64, 15, recv.at[15, 0])
        once = {0: 15 * 8, 1: 7, 2: 7, 3: 15 * 8, 4: 3 * 8 * 8, 5: 2 * 3 * 4 * 2, 10: 2 * 3 * 8 * 2, 6: 15 * 3}
        for stage, count in once.items():
            sent(CHUNKS * count, stage)
        for stage, count in {7: 15, 8: 16, 11: 16, 12: 16}.items():
            sent(s * count, stage)
        sent(s * 64, 9)
        for stage, count in {13: 3, 14: 6, 16: 6, 17: 48, 15: 64}.items():
            sent(rest * count, stage)

    def load():
        for k in range(CHUNKS):
            own_color(k).start()
        for cp in ranks:
            cp.wait()
        tab.extend(tables())

    tab = []
    stages = dict(alpha=alpha, prefix=prefix, group=group, trans=trans, scale=scale, sum_core=sum_core, around=around, sum_y=sum_y,
                  sum_xz=sum_xz, gather_y=gather_y, forward=forward, gather_core=gather_core, spread=spread, cross=cross,
                  spread_core=spread_core)
    ranks = [pltpu.make_async_copy(depth_in, depth, own.at[2, 0]), pltpu.make_async_copy(bricks_in, bricks, own.at[2, 1])]
    for cp in ranks:
        cp.start()
    meet()
    for name in PLAN:
        with jax.named_scope(name):
            if name == "load":
                load()
            elif name == "finish":
                finish()
            elif name[-1] == "a":
                alpha(int(name[-2]), 0, 7)
            elif name[-1] == "b":
                alpha(int(name[-2]), 7, 15)
            else:
                stages[name[:-1]](int(name[-1]))


def local(images, depth, brick_map):
    channels, rows, columns = images.shape[1:]
    width = columns // CHUNKS
    tile, half = width // 8, width // 2
    f = jnp.float32
    n = CHUNKS
    vm = lambda *s: pltpu.VMEM(s, f)
    out = pl.pallas_call(
        kernel,
        out_shape=pltpu.VMEM((channels, 2, 2, 4, ROW, columns), f),
        in_specs=[pl.BlockSpec(memory_space=pl.ANY)] * 3,
        out_specs=pl.BlockSpec(memory_space=pltpu.VMEM),
        scratch_shapes=[
            *[vm(16, ROW, width)] * n, *[vm(8, ROW, tile)] * n,
            vm(n, 16, ROW, width), vm(n, 8, ROW, tile), vm(n, 8, ROW, tile), vm(n, 8, ROW, tile), vm(n, 8, ROW, tile),
            vm(n, 16, ROW, width), vm(n, 16, ROW, width),
            vm(n, 3, 2, 2, 4, ROW, width), vm(n, 3, 8, ROW, width), vm(n, 3, 8, ROW, width), vm(n, 3, 8, 2, ROW, half),
            vm(n, 2, 3, 4, 2, ROW, tile), vm(n, 2, 3, 4, 2, ROW, tile), vm(n, 2, 3, 8, 2, ROW, tile), vm(n, 3, 8, 2, ROW, tile), vm(n, 15, 3, ROW, tile),
            pltpu.SemaphoreType.DMA((18,)), pltpu.SemaphoreType.DMA((18, n)), pltpu.SemaphoreType.DMA((3, n)),
            pltpu.SMEM(depth.shape, jnp.int32), pltpu.SMEM(brick_map.shape, jnp.int32),
        ],
        compiler_params=pltpu.CompilerParams(has_side_effects=True, collective_id=0, vmem_limit_bytes=48 * 2**20),
    )(depth, brick_map, images.reshape(channels, 2, 2, 4, ROW, columns))
    return out.reshape(channels, rows, columns)


def solution(mesh):
    torus = Mesh(mesh.devices.reshape(2, 4, 2, 2, 4), AXES)
    return jax.shard_map(
        local,
        mesh=torus,
        in_specs=(P(("zh", "x", "c", "zl", "y"), None, None, None), P(), P()),
        out_specs=P(),
        check_vma=False,
    )
```
